32 devices in a mesh: pert: 2 (over x), ga: 16 (over z, y, core).
Axes of the slice: x: 2, y: 2, z: 4, core: 2. Of those that a mesh axis runs over, the one named last changes fastest.
Arguments:
- psi_k: bfloat16 [2, 8192, 256], P(None, 'ga'), may hold values from -6 to 6
- beta_k: bfloat16 [2, 8192, 2496], P(None, 'ga'), may hold values from -0.0625 to 0.0625
- beta_kq: bfloat16 [2, 8192, 2496], P(None, 'ga'), may hold values from -0.15625 to 0.15625
- g_k: float32 [3, 8192], P(None, 'ga'), may hold values from -2 to 2
- g_kq: float32 [3, 8192], P(None, 'ga'), may hold values from -2 to 2
- send_index: int32 [16, 16, 32], P('ga'), may hold values from -1 to 511, as said below
- recv_index: int32 [8192], P('ga'), may hold values from -1 to 511, as said below
- dmat: float32 [192, 13, 13], replicated, may hold values from -0.5 to 4, as said below
- displaced: int32 [256], P('pert'), parts along dimension 0, may hold values from 0 to 191, as said below
- mode: float32 [3, 256], P(None, 'pert'), parts along dimension 1, may hold values from -5 to 5
Outputs:
- dvpsi: bfloat16 [4, 8192, 256], P('pert', 'ga'), parts along dimension 0
The draws below stay inside these ranges and needn't reach their ends.
There are 2 independent parts, one for each index of `pert`. The reference program is written for one: setup_inputs(seed, part) draws one part's arguments, and reference() takes and returns one part's arrays. A program takes and returns all parts, laid end to end along the dimension named above; an argument that names none is the same for every part. Nothing has to cross between parts.
Inputs may be any that keep to these rules, and one draw needn't show every extreme that they name: `send_index`: entry [s, d, c] is a row of device s's k-sphere block in local numbering, or -1 for an unused slot; the rows device s sends are distinct; in every draw some device receives 32 rows from every device. `recv_index`: entry r is s * 32 + c, naming slot c from device s among the rows received by the device of row r, or -1 for a row with no k-sphere counterpart; every used slot is named by exactly one row of its receiving device and no unused slot is named. `dmat`: each atom's block is symmetric. `displaced`: 128 distinct atoms.
All inputs are finite; a program needn't handle non-finite values.
Results may differ from the reference program's by a relative error of at most 0.0057.
Values may be sent and summed in bfloat16 or wider, within the bound.
A program may use at most 128 MiB of HBM per device.

```python
import jax
import jax.numpy as jnp
from jax import lax

KQ_DEV = 512
NB = 256
NPROJ_ATOM = 13
ATOMS = 192
DISP = 128
CAP = 32
NPW_Q = 8192
NPROJ = 2496
N_GA = 16


def exchange_plan(key):
    base = jax.random.fold_in(key, 7)
    key_counts, key_full, key_send, key_rows = jax.random.split(base, 4)
    short_draw = jax.random.randint(key_counts, (N_GA, N_GA), 0, 10)
    counts = jnp.where(short_draw == 0, CAP - 1, CAP)
    full_target = jax.random.randint(key_full, (), 0, N_GA)
    counts = jnp.where(jnp.arange(N_GA)[None, :] == full_target, CAP, counts).astype(jnp.int32)
    send_order = jax.vmap(lambda single: jax.random.permutation(single, KQ_DEV))(jax.random.split(key_send, N_GA)).astype(jnp.int32)
    slot_ids = jnp.arange(CAP, dtype=jnp.int32)
    offsets = jnp.cumsum(counts, axis=1) - counts
    positions = jnp.minimum(offsets[:, :, None] + slot_ids[None, None, :], KQ_DEV - 1).reshape(N_GA, N_GA * CAP)
    sent_rows = jnp.take_along_axis(send_order, positions, axis=1).reshape(N_GA, N_GA, CAP)
    live_slots = slot_ids[None, None, :] < counts[:, :, None]
    send_table = jnp.where(live_slots, sent_rows, -1).astype(jnp.int32)
    live_dest = jnp.transpose(live_slots, (1, 0, 2)).reshape(N_GA, N_GA * CAP)
    live_order = jnp.argsort(jnp.where(live_dest, 0, 1).astype(jnp.int32), axis=1, stable=True).astype(jnp.int32)
    live_total = jnp.sum(live_dest.astype(jnp.int32), axis=1)
    padded_order = jnp.concatenate([live_order, jnp.zeros((N_GA, KQ_DEV - N_GA * CAP), jnp.int32)], axis=1)
    row_ids = jnp.arange(KQ_DEV, dtype=jnp.int32)
    buffer_vals = jnp.where(row_ids[None, :] < live_total[:, None], padded_order, -1).astype(jnp.int32)
    row_perms = jax.vmap(lambda single: jax.random.permutation(single, KQ_DEV))(jax.random.split(key_rows, N_GA)).astype(jnp.int32)
    recv_table = jnp.zeros((N_GA, KQ_DEV), jnp.int32).at[jnp.arange(N_GA)[:, None], row_perms].set(buffer_vals)
    return (send_table, recv_table.reshape(-1))


def draw_send_index(key, part):
    send_table, recv_table = exchange_plan(key)
    return send_table


def draw_recv_index(key, part):
    send_table, recv_table = exchange_plan(key)
    return recv_table


def draw_dmat(key, part):
    key_off, key_diag = jax.random.split(jax.random.fold_in(key, 11))
    raw = jnp.clip(0.3 * jax.random.normal(key_off, (ATOMS, NPROJ_ATOM, NPROJ_ATOM), jnp.float32), -0.5, 0.5)
    symmetric = 0.5 * (raw + jnp.swapaxes(raw, 1, 2))
    diagonal = jax.random.uniform(key_diag, (ATOMS, NPROJ_ATOM), jnp.float32, 0.5, 2.5)
    identity = jnp.eye(NPROJ_ATOM, dtype=jnp.float32)
    return symmetric * (1.0 - identity) + diagonal[:, :, None] * identity


def draw_displaced(key, part):
    chosen = jax.random.permutation(jax.random.fold_in(key, 13), ATOMS)
    return chosen[:DISP].astype(jnp.int32)


def shard_levels(stream_key, shape, cuts, smallest, high):
    loudness = 1.0
    for dim, parts in cuts:
        steps = jax.random.uniform(jax.random.fold_in(jax.random.fold_in(stream_key, 6), dim), (parts,), jnp.float32, smallest / len(cuts), high / len(cuts))
        loudness = loudness * jnp.repeat(jnp.exp(steps), shape[dim] // parts).reshape((-1,) + (1,) * (len(shape) - 1 - dim))
    return loudness


def bell_draw(key, shape, deviation, most, cuts=(), kind=jnp.bfloat16):
    result = jax.random.normal(key, shape, jnp.float32) * deviation
    if len(cuts) > 0:
        result = shard_levels(key, shape, cuts, -0.22, 0.18) * result
    return jnp.clip(result, min=-most, max=most).astype(kind)


def setup_inputs(seed: int = 0, part: int = 0) -> dict:
    arg_keys = jax.random.split(jax.random.key(seed), 11)
    own_keys = jax.random.split(jax.random.fold_in(arg_keys[10], part), 11)
    psi_k = bell_draw(arg_keys[0], (2, NPW_Q, NB), 1.0, 6.0, ((1, 16),))
    beta_k = bell_draw(arg_keys[1], (2, NPW_Q, NPROJ), NPW_Q ** -0.5, 0.0625, ((1, 16),))
    beta_kq = bell_draw(arg_keys[2], (2, NPW_Q, NPROJ), (DISP * NPROJ_ATOM) ** -0.5, 0.15625, ((1, 16),))
    g_k = jnp.clip(jax.random.uniform(arg_keys[3], (3, NPW_Q), jnp.float32, -2.0, 2.0) * shard_levels(arg_keys[3], (3, NPW_Q), ((1, 16),), -0.4, 0.0), -2.0, 2.0)
    g_kq = jnp.clip(jax.random.uniform(arg_keys[4], (3, NPW_Q), jnp.float32, -2.0, 2.0) * shard_levels(arg_keys[4], (3, NPW_Q), ((1, 16),), -0.4, 0.0), -2.0, 2.0)
    send_index = draw_send_index(jax.random.fold_in(arg_keys[10], 71), part)
    recv_index = draw_recv_index(jax.random.fold_in(arg_keys[10], 71), part)
    dmat = draw_dmat(jax.random.fold_in(arg_keys[10], 71), part)
    displaced = draw_displaced(jax.random.fold_in(jax.random.fold_in(arg_keys[10], part), 71), part)
    mode = bell_draw(own_keys[9], (3, DISP), 1.0, 5.0, (), jnp.float32)
    return dict(psi_k=psi_k, beta_k=beta_k, beta_kq=beta_kq, g_k=g_k, g_kq=g_kq, send_index=send_index, recv_index=recv_index, dmat=dmat, displaced=displaced, mode=mode)


def contract_rows(left_side, stacked):
    return lax.dot_general(left_side, stacked, (((0,), (0,)), ((), ())), preferred_element_type=jnp.float32)


def local_terms(wave_rows, beta_rows, g_vectors, columns, weights):
    band_count = wave_rows.shape[2]
    picked = jnp.take(beta_rows, columns, axis=2)
    row_scale = jnp.dot(g_vectors.T, weights, precision=lax.Precision.HIGHEST, preferred_element_type=jnp.float32)
    conj_real = (row_scale * picked[1]).astype(jnp.bfloat16)
    conj_imag = (row_scale * picked[0]).astype(jnp.bfloat16)
    stacked = jnp.concatenate([wave_rows[0], wave_rows[1]], axis=1)
    with_real = contract_rows(picked[0], stacked)
    with_imag = contract_rows(picked[1], stacked)
    slope_real = contract_rows(conj_real, stacked)
    slope_imag = contract_rows(conj_imag, stacked)
    plain_part = jnp.stack([with_real[:, :band_count] + with_imag[:, band_count:],
                            with_real[:, band_count:] - with_imag[:, :band_count]])
    slope_part = jnp.stack([slope_real[:, :band_count] - slope_imag[:, band_count:],
                            slope_real[:, band_count:] + slope_imag[:, :band_count]])
    return jnp.stack([plain_part, slope_part])


def couple_atoms(summed, coupling):
    shape_in = summed.shape
    blocks = summed.reshape(2, 2, coupling.shape[0], coupling.shape[1], shape_in[3])
    mixed = jnp.einsum("dij,xcdjn->xcdin", coupling, blocks, precision=lax.Precision.HIGHEST)
    return mixed.reshape(shape_in).astype(jnp.bfloat16)


def back_project(coupled, beta_rows, g_vectors, columns, weights):
    band_count = coupled.shape[3]
    picked = jnp.take(beta_rows, columns, axis=2)
    row_scale = jnp.dot(g_vectors.T, weights, precision=lax.Precision.HIGHEST, preferred_element_type=jnp.float32)
    slope_real = (row_scale * picked[1]).astype(jnp.bfloat16)
    slope_imag = (-row_scale * picked[0]).astype(jnp.bfloat16)
    left_side = jnp.concatenate([slope_real, slope_imag, picked[0], picked[1]], axis=1)
    bra_terms = coupled[0]
    ket_terms = coupled[1]
    real_part = jnp.concatenate([bra_terms[0], -bra_terms[1], ket_terms[0], -ket_terms[1]], axis=0)
    imag_part = jnp.concatenate([bra_terms[1], bra_terms[0], ket_terms[1], ket_terms[0]], axis=0)
    right_side = jnp.concatenate([real_part, imag_part], axis=1)
    product = jnp.dot(left_side, right_side, preferred_element_type=jnp.float32)
    return jnp.stack([product[:, :band_count], product[:, band_count:]]).astype(jnp.bfloat16)


def reference(psi_k, beta_k, beta_kq, g_k, g_kq, send_index, recv_index, dmat, displaced, mode):
    row_total = recv_index.shape[0]
    row_ids = jnp.arange(row_total, dtype=jnp.int32)
    target = (row_ids // KQ_DEV).astype(jnp.int32)
    buffer_pos = jnp.maximum(recv_index, 0).astype(jnp.int32)
    source = (buffer_pos // CAP).astype(jnp.int32)
    slot_ids = (buffer_pos % CAP).astype(jnp.int32)
    local_row = send_index[source, target, slot_ids]
    live_rows = (recv_index >= 0) & (local_row >= 0)
    anchor = (source * KQ_DEV + jnp.maximum(local_row, 0)).astype(jnp.int32)
    psi_kq = jnp.where(live_rows[None, :, None], psi_k[:, anchor, :], jnp.zeros((), psi_k.dtype))
    columns = (displaced[:, None] * NPROJ_ATOM + jnp.arange(NPROJ_ATOM, dtype=jnp.int32)[None, :]).reshape(-1).astype(jnp.int32)
    atom_of = jnp.repeat(jnp.arange(DISP, dtype=jnp.int32), NPROJ_ATOM)
    weights = mode[:, atom_of]
    proj_count = columns.shape[0]

    def project_block(running, block_id):
        row_start = (block_id * KQ_DEV).astype(jnp.int32)
        wave_rows = lax.dynamic_slice_in_dim(psi_kq, row_start, KQ_DEV, 1)
        beta_rows = lax.dynamic_slice_in_dim(beta_k, row_start, KQ_DEV, 1)
        g_vectors = lax.dynamic_slice_in_dim(g_k, row_start, KQ_DEV, 1)
        return running + local_terms(wave_rows, beta_rows, g_vectors, columns, weights), None

    start_sum = jnp.zeros((2, 2, proj_count, NB), jnp.float32)
    summed, unused = lax.scan(project_block, start_sum, jnp.arange(N_GA, dtype=jnp.int32))
    coupling = jnp.take(dmat, displaced, axis=0)
    coupled = couple_atoms(summed, coupling)

    def apply_block(block_id):
        row_start = (block_id * KQ_DEV).astype(jnp.int32)
        beta_rows = lax.dynamic_slice_in_dim(beta_kq, row_start, KQ_DEV, 1)
        g_vectors = lax.dynamic_slice_in_dim(g_kq, row_start, KQ_DEV, 1)
        return back_project(coupled, beta_rows, g_vectors, columns, weights)

    pieces = lax.map(apply_block, jnp.arange(N_GA, dtype=jnp.int32))
    return jnp.transpose(pieces, (1, 0, 2, 3)).reshape(2, row_total, NB)
```

```python
import functools

import jax
import jax.numpy as jnp
from jax import lax
from jax.experimental import pallas as pl
from jax.experimental.pallas import tpu as pltpu
from jax.sharding import PartitionSpec as P

LANES = 128
BF16 = jnp.bfloat16
F32 = jnp.float32
VMEM_LIMIT = 56 * 1024 * 1024


def round_up(value, step):
    return -(-value // step) * step


def dot(a, b):
    return jnp.dot(a, b, preferred_element_type=F32)


def dot_t(a, b):
    return lax.dot_general(a, b, (((0,), (0,)), ((), ())), preferred_element_type=F32)


def pack_kernel(slot_ref, psi_ref, out_ref):
    rows = psi_ref.shape[1]
    bands = psi_ref.shape[2]
    slots = slot_ref.shape[1]
    pick = (lax.broadcasted_iota(jnp.int32, (rows, slots), 0) == slot_ref[...]).astype(BF16)
    for part in range(2):
        out_ref[:, part * bands:(part + 1) * bands] = dot_t(pick, psi_ref[part]).astype(BF16)


def pack_rows(slots, psi_k):
    return pl.pallas_call(
        pack_kernel,
        out_shape=jax.ShapeDtypeStruct((slots.shape[1], 2 * psi_k.shape[2]), BF16),
        compiler_params=pltpu.CompilerParams(vmem_limit_bytes=VMEM_LIMIT),
    )(slots, psi_k)


class Layout:
    def __init__(self, groups, atoms, per_atom, total):
        self.groups = groups
        self.per_shard = atoms // groups
        self.per_atom = per_atom
        self.used = self.per_shard * per_atom
        self.rows = round_up(self.used, 16)
        self.columns = groups * self.rows
        self.total = total
        self.block = 2 * LANES if self.columns % (2 * LANES) == 0 else self.columns
        slack = total - atoms * per_atom
        need = 0
        for t in range(self.columns // self.block):
            low = self.first(t * self.block)
            high = self.first((t + 1) * self.block - 1)
            need = max(need, high - low // LANES * LANES + slack + 1)
        self.last_start = max(0, (total - need) // LANES * LANES)
        self.window = total - self.last_start

    def first(self, column):
        inside = column % self.rows
        return column // self.rows * self.used + min(inside, self.used - 1)

    def start(self, t):
        column = t * self.block
        low = column // self.rows * self.used + jnp.minimum(column % self.rows, self.used - 1)
        low = jnp.minimum(low // LANES * LANES, self.last_start)
        return pl.multiple_of(low, LANES)


def select(layout, beta_ref, source_ref, t):
    start = layout.start(t)
    ids = lax.broadcasted_iota(jnp.int32, (layout.window, layout.block), 0) + start
    pick = (ids == source_ref[...]).astype(BF16)
    return dot(beta_ref[:, pl.ds(start, layout.window)], pick).astype(BF16)


def row_scale(g_ref, weight_ref):
    total = g_ref[:, 0:1] * weight_ref[0:1, :]
    for x in range(1, g_ref.shape[1]):
        total = total + g_ref[:, x:x + 1] * weight_ref[x:x + 1, :]
    return total


def project_kernel(layout, arrived_ref, slot_ref, beta_ref, source_ref, weight_ref, g_ref, out_ref, wave):
    t = pl.program_id(0)
    rows = wave.shape[0]
    bands = wave.shape[1] // 2

    @pl.when(t == 0)
    def _():
        slots = arrived_ref.shape[0]
        pick = (lax.broadcasted_iota(jnp.int32, (slots, rows), 0) == slot_ref[...]).astype(BF16)
        wave[...] = dot_t(pick, arrived_ref[...]).astype(BF16)

    picked = select(layout, beta_ref, source_ref, t)
    scale = row_scale(g_ref, weight_ref)
    real, imag = picked[:rows], picked[rows:]
    conj_real = (scale * imag).astype(BF16)
    conj_imag = (scale * real).astype(BF16)
    stacked = wave[...]
    a = dot_t(real, stacked)
    b = dot_t(imag, stacked)
    out_ref[:, :bands] = (a[:, :bands] + b[:, bands:]).astype(BF16)
    out_ref[:, bands:2 * bands] = (a[:, bands:] - b[:, :bands]).astype(BF16)
    a = dot_t(conj_real, stacked)
    b = dot_t(conj_imag, stacked)
    out_ref[:, 2 * bands:3 * bands] = (a[:, :bands] - b[:, bands:]).astype(BF16)
    out_ref[:, 3 * bands:] = (a[:, bands:] + b[:, :bands]).astype(BF16)


def whole_block(shape):
    return pl.BlockSpec(shape, lambda t: (0,) * len(shape))


def project(layout, arrived, slots, beta, source, weights, g):
    rows, width = slots.shape[1], arrived.shape[1]
    block = layout.block
    return pl.pallas_call(
        functools.partial(project_kernel, layout),
        grid=(layout.columns // block,),
        in_specs=[
            whole_block(arrived.shape),
            whole_block(slots.shape),
            whole_block(beta.shape),
            pl.BlockSpec((1, block), lambda t: (0, t)),
            pl.BlockSpec((weights.shape[0], block), lambda t: (0, t)),
            whole_block(g.shape),
        ],
        out_specs=pl.BlockSpec((block, 2 * width), lambda t: (t, 0)),
        out_shape=jax.ShapeDtypeStruct((layout.columns, 2 * width), BF16),
        scratch_shapes=[pltpu.VMEM((rows, width), BF16)],
        compiler_params=pltpu.CompilerParams(vmem_limit_bytes=VMEM_LIMIT),
    )(arrived, slots, beta, source, weights, g)


def prepare_kernel(layout, beta_ref, source_ref, weight_ref, g_ref, out_ref):
    rows = g_ref.shape[0]
    picked = select(layout, beta_ref, source_ref, pl.program_id(0))
    scale = row_scale(g_ref, weight_ref)
    real, imag = picked[:rows], picked[rows:]
    out_ref[0] = (scale * imag).astype(BF16)
    out_ref[1] = (-scale * real).astype(BF16)
    out_ref[2] = real
    out_ref[3] = imag


def prepare(layout, beta, source, weights, g):
    block = layout.block
    rows = g.shape[0]
    flops = 2 * beta.shape[0] * layout.window * layout.columns
    return pl.pallas_call(
        functools.partial(prepare_kernel, layout),
        grid=(layout.columns // block,),
        in_specs=[
            whole_block(beta.shape),
            pl.BlockSpec((1, block), lambda t: (0, t)),
            pl.BlockSpec((weights.shape[0], block), lambda t: (0, t)),
            whole_block(g.shape),
        ],
        out_specs=pl.BlockSpec((4, rows, block), lambda t: (0, 0, t)),
        out_shape=jax.ShapeDtypeStruct((4, rows, layout.columns), BF16),
        cost_estimate=pl.CostEstimate(
            flops=flops, bytes_accessed=2 * beta.size + 8 * rows * layout.columns, transcendentals=0
        ),
        compiler_params=pltpu.CompilerParams(vmem_limit_bytes=VMEM_LIMIT),
    )(beta, source, weights, g)


def back_kernel(left_ref, coupled_ref, out_ref, total):
    t = pl.program_id(0)
    bands = out_ref.shape[2]
    first = coupled_ref[:, :2 * bands]
    second = coupled_ref[:, 2 * bands:]
    a = dot(left_ref[0], first) + dot(left_ref[2], second)
    b = dot(left_ref[1], first) + dot(left_ref[3], second)
    real = a[:, :bands] - b[:, bands:]
    imag = a[:, bands:] + b[:, :bands]

    @pl.when(t == 0)
    def _():
        total[0] = real
        total[1] = imag

    @pl.when(t > 0)
    def _():
        total[0] += real
        total[1] += imag

    @pl.when(t == pl.num_programs(0) - 1)
    def _():
        out_ref[...] = total[...].astype(BF16)


def back_project(layout, left, coupled):
    block = layout.block
    rows = left.shape[1]
    bands = coupled.shape[1] // 4
    return pl.pallas_call(
        back_kernel,
        grid=(layout.columns // block,),
        in_specs=[
            pl.BlockSpec((4, rows, block), lambda t: (0, 0, t)),
            pl.BlockSpec((block, 4 * bands), lambda t: (t, 0)),
        ],
        out_specs=pl.BlockSpec((2, rows, bands), lambda t: (0, 0, 0)),
        out_shape=jax.ShapeDtypeStruct((2, rows, bands), BF16),
        scratch_shapes=[pltpu.VMEM((2, rows, bands), F32)],
        compiler_params=pltpu.CompilerParams(vmem_limit_bytes=VMEM_LIMIT),
    )(left, coupled)


def spread(layout, values, step, fill):
    lead = values.shape[:-1]
    parts = values.reshape(lead + (layout.groups, layout.per_shard))
    parts = jnp.repeat(parts, layout.per_atom, axis=-1)
    parts = parts * step + jnp.tile(jnp.arange(layout.per_atom, dtype=parts.dtype), layout.per_shard) * (
        1 if step != 1 else 0
    )
    pads = [(0, 0)] * len(lead) + [(0, 0), (0, layout.rows - layout.used)]
    return jnp.pad(parts, pads, constant_values=fill).reshape(lead + (layout.columns,))


def block_coupling(layout, dmat, atoms):
    mine = lax.dynamic_slice_in_dim(atoms, lax.axis_index("ga") * layout.per_shard, layout.per_shard)
    blocks = jnp.take(dmat, mine, axis=0)
    eye = jnp.eye(layout.per_shard, dtype=F32)
    full = (blocks[:, :, None, :] * eye[:, None, :, None]).reshape(layout.used, layout.used)
    extra = layout.rows - layout.used
    return jnp.pad(full, ((0, extra), (0, extra)))


def on_device(psi_k, beta_k, beta_kq, g_k, g_kq, send_index, recv_index, dmat, displaced, mode):
    groups = lax.axis_size("ga")
    total = beta_k.shape[2]
    rows = beta_k.shape[1]
    per_atom = dmat.shape[1]
    layout = Layout(groups, displaced.shape[0], per_atom, total)

    packed = pack_rows(send_index.reshape(1, -1), psi_k)
    arrived = lax.all_to_all(packed, "ga", split_axis=0, concat_axis=0, tiled=True)

    rank = jnp.sum((displaced[None, :] < displaced[:, None]).astype(jnp.int32), axis=1)
    place = rank[None, :] == jnp.arange(displaced.shape[0], dtype=jnp.int32)[:, None]
    atoms = jnp.sum(jnp.where(place, displaced[None, :], 0), axis=1)
    moves = jnp.sum(jnp.where(place[None], mode[:, None, :], 0.0), axis=2)
    source = spread(layout, atoms, per_atom, -1).reshape(1, -1)
    weights = spread(layout, moves, 1, 0)

    partial_terms = project(
        layout, arrived, recv_index.reshape(1, -1), beta_k.reshape(2 * rows, total), source, weights, g_k.T
    )
    shard = lax.psum_scatter(partial_terms, "ga", scatter_dimension=0, tiled=True)
    left = prepare(layout, beta_kq.reshape(2 * rows, total), source, weights, g_kq.T)
    coupling = block_coupling(layout, dmat, atoms)
    mixed = jnp.dot(
        coupling, shard.astype(F32), precision=lax.Precision.HIGHEST, preferred_element_type=F32
    ).astype(BF16)
    coupled = lax.all_gather(mixed, "ga", axis=0, tiled=True)
    return back_project(layout, left, coupled)


def solution(mesh):
    in_specs = (
        P(None, "ga", None),
        P(None, "ga", None),
        P(None, "ga", None),
        P(None, "ga"),
        P(None, "ga"),
        P("ga", None, None),
        P("ga"),
        P(),
        P("pert"),
        P(None, "pert"),
    )
    out_specs = P("pert", "ga", None)
    return jax.shard_map(
        on_device, mesh=mesh, in_specs=in_specs, out_specs=out_specs, check_vma=False
    )
```

```python
import functools

import jax
import jax.numpy as jnp
from jax import lax
from jax.experimental import pallas as pl
from jax.experimental.pallas import tpu as pltpu
from jax.sharding import PartitionSpec as P

LANES = 128
RING = 4
CORE_Y = 4
BF16 = jnp.bfloat16
F32 = jnp.float32
VMEM_LIMIT = 56 * 1024 * 1024


def round_up(value, step):
    return -(-value // step) * step


def dot(a, b):
    return jnp.dot(a, b, preferred_element_type=F32)


def dot_t(a, b):
    return lax.dot_general(a, b, (((0,), (0,)), ((), ())), preferred_element_type=F32)


def pack_kernel(slot_ref, psi_ref, out_ref):
    rows = psi_ref.shape[1]
    bands = psi_ref.shape[2]
    slots = slot_ref.shape[1]
    pick = (lax.broadcasted_iota(jnp.int32, (rows, slots), 0) == slot_ref[...]).astype(BF16)
    for part in range(2):
        out_ref[:, part * bands:(part + 1) * bands] = dot_t(pick, psi_ref[part]).astype(BF16)


def pack_rows(slots, psi_k):
    return pl.pallas_call(
        pack_kernel,
        out_shape=jax.ShapeDtypeStruct((slots.shape[1], 2 * psi_k.shape[2]), BF16),
        compiler_params=pltpu.CompilerParams(vmem_limit_bytes=VMEM_LIMIT),
    )(slots, psi_k)


class Layout:
    def __init__(self, groups, atoms, per_atom, total):
        self.groups = groups
        self.blocks = groups // CORE_Y
        self.gang = CORE_Y
        if self.blocks != RING:
            self.blocks = RING
            self.gang = groups // RING
        self.per_shard = atoms // groups
        self.per_atom = per_atom
        self.used = self.per_shard * per_atom
        self.rows = round_up(self.used, 16)
        self.block = self.gang * self.rows
        self.padded = round_up(self.block, LANES)
        self.total = total
        slack = total - atoms * per_atom
        self.window = min(total, round_up(self.gang * self.used + slack + 16, LANES))
        self.starts = [
            min(b * self.gang * self.used // 16 * 16, total - self.window) for b in range(self.blocks)
        ]


def columns_of(layout, info_ref, b):
    wide = info_ref[:, b * layout.padded:(b + 1) * layout.padded]
    return jnp.transpose(wide)[: layout.block]


def select(layout, beta_ref, info, b):
    start = layout.starts[b]
    ids = lax.broadcasted_iota(jnp.int32, (layout.block, layout.window), 1) + start
    pick = (ids == info[:, 0:1].astype(jnp.int32)).astype(BF16)
    rows = pl.ds(start, layout.window)
    return dot(pick, beta_ref[0, rows, :]), dot(pick, beta_ref[1, rows, :])


def row_scale(g_ref, info):
    total = info[:, 1:2] * g_ref[0:1, :]
    for x in range(1, g_ref.shape[0]):
        total = total + info[:, x + 1:x + 2] * g_ref[x:x + 1, :]
    return total


def regroup(arrived_ref, slot_ref, wave):
    slots, rows = arrived_ref.shape[0], wave.shape[0]
    pick = (lax.broadcasted_iota(jnp.int32, (slots, rows), 0) == slot_ref[...]).astype(BF16)
    wave[...] = dot_t(pick, arrived_ref[...]).astype(BF16)


def project_block(layout, beta_ref, info_ref, g_ref, wave, store, b):
    bands = wave.shape[1] // 2
    info = columns_of(layout, info_ref, b)
    real, imag = select(layout, beta_ref, info, b)
    scale = row_scale(g_ref, info)
    stacked = wave[...]
    x = dot(real.astype(BF16), stacked)
    y = dot(imag.astype(BF16), stacked)
    store(0, (x[:, :bands] + y[:, bands:]).astype(BF16))
    store(1, (x[:, bands:] - y[:, :bands]).astype(BF16))
    x = dot((scale * imag).astype(BF16), stacked)
    y = dot((scale * real).astype(BF16), stacked)
    store(2, (x[:, :bands] - y[:, bands:]).astype(BF16))
    store(3, (x[:, bands:] + y[:, :bands]).astype(BF16))


def prepare_block(layout, beta_ref, info_ref, g_ref, left_ref, b):
    info = columns_of(layout, info_ref, b)
    real, imag = select(layout, beta_ref, info, b)
    scale = row_scale(g_ref, info)
    for k, term in enumerate((scale * imag, -scale * real, real, imag)):
        left_ref[b, k] = term.astype(BF16).T


def back_block(left_ref, b, coupled):
    width = coupled.shape[1] // 2
    bands = width // 2
    first, second = coupled[:, :width], coupled[:, width:]
    x = dot(left_ref[b, 0], first) + dot(left_ref[b, 2], second)
    y = dot(left_ref[b, 1], first) + dot(left_ref[b, 3], second)
    return x[:, :bands] - y[:, bands:], x[:, bands:] + y[:, :bands]


def project_kernel(layout, arrived_ref, slot_ref, beta_ref, info_ref, g_ref, out_ref, wave):
    regroup(arrived_ref, slot_ref, wave)
    bands = wave.shape[1] // 2
    for b in range(layout.blocks):

        def store(k, value, b=b):
            out_ref[b * layout.block:(b + 1) * layout.block, k * bands:(k + 1) * bands] = value

        project_block(layout, beta_ref, info_ref, g_ref, wave, store, b)


def finish_kernel(layout, beta_ref, info_ref, g_ref, coupled_ref, out_ref, left, total):
    for b in range(layout.blocks):
        prepare_block(layout, beta_ref, info_ref, g_ref, left, b)
        parts = back_block(left, b, coupled_ref[b * layout.block:(b + 1) * layout.block, :])
        for k in range(2):
            total[k] = parts[k] if b == 0 else total[k] + parts[k]
    out_ref[...] = total[...].astype(BF16)


def params(**extra):
    return pltpu.CompilerParams(vmem_limit_bytes=VMEM_LIMIT, **extra)


def separate_steps(layout, arrived, slots, beta_k, beta_kq, info, g_k, g_kq, coupling):
    rows, width = slots.shape[1], arrived.shape[1]
    terms = pl.pallas_call(
        functools.partial(project_kernel, layout),
        out_shape=jax.ShapeDtypeStruct((layout.groups * layout.rows, 2 * width), BF16),
        scratch_shapes=[pltpu.VMEM((rows, width), BF16)],
        compiler_params=params(),
    )(arrived, slots, beta_k, info, g_k)
    shard = lax.psum_scatter(terms.astype(F32), "ga", scatter_dimension=0, tiled=True)
    mixed = jnp.dot(
        coupling, shard, precision=lax.Precision.HIGHEST, preferred_element_type=F32
    ).astype(BF16)
    coupled = lax.all_gather(mixed, "ga", axis=0, tiled=True)
    return pl.pallas_call(
        functools.partial(finish_kernel, layout),
        out_shape=jax.ShapeDtypeStruct((2, rows, width // 2), BF16),
        scratch_shapes=[
            pltpu.VMEM((layout.blocks, 4, rows, layout.block), BF16),
            pltpu.VMEM((2, rows, width // 2), F32),
        ],
        compiler_params=params(),
    )(beta_kq, info, g_kq, coupled)


class Sends:
    def __init__(self, send_sem, recv_sem):
        self.send_sem, self.recv_sem = send_sem, recv_sem
        self.started = []

    def start(self, source, target, device):
        k = len(self.started)
        copy = pltpu.make_async_remote_copy(
            src_ref=source,
            dst_ref=target,
            send_sem=self.send_sem.at[k],
            recv_sem=self.recv_sem.at[k],
            device_id={"ga": device},
            device_id_type=pl.DeviceIdType.MESH,
        )
        copy.start()
        self.started.append(copy)
        return copy

    def finish(self):
        for copy in self.started:
            copy.wait_send()


def fused_kernel(
    layout, arrived_ref, slot_ref, beta_k_ref, info_ref, g_k_ref, g_kq_ref, coupling_ref, beta_kq_hbm,
    out_ref, wave, part, core_in, mine, y_in, y_sum, za_in, za_mid, zb_in, zb_mid, b_sum, b_in,
    coupled, left, total, beta_kq, send_sem, recv_sem, load_sem,
):
    me = lax.axis_index("ga")
    c, y, z = me % 2, (me // 2) % 2, me // 4

    def index(zz, yy, cc):
        return (zz * 2 + yy) * 2 + cc

    up, down, far = (z + 1) % RING, (z + RING - 1) % RING, (z + 2) % RING
    other_core, other_y = index(z, y, 1 - c), index(z, 1 - y, c)
    next_z, last_z = index(up, y, c), index(down, y, c)
    load = pltpu.make_async_copy(beta_kq_hbm, beta_kq, load_sem)
    load.start()

    barrier = pltpu.get_barrier_semaphore()
    partners = (other_core, other_y, next_z, last_z)
    for partner in partners:
        pl.semaphore_signal(barrier, inc=1, device_id={"ga": partner}, device_id_type=pl.DeviceIdType.MESH)
    pl.semaphore_wait(barrier, len(partners))

    sends = Sends(send_sem, recv_sem)
    rows = layout.rows
    bands = wave.shape[1] // 2
    half = 2 * bands
    low, high = pl.ds(0, half), pl.ds(half, half)
    left_cols, right_cols = pl.ds(0, bands), pl.ds(bands, bands)
    high_left, high_right = pl.ds(half, bands), pl.ds(half + bands, bands)

    def add(first, *others):
        value = first.astype(F32)
        for other in others:
            value = value + other.astype(F32)
        return value

    regroup(arrived_ref, slot_ref, wave)
    core_copies = []
    for b in range(RING):

        def store(k, value, b=b):
            for yy in range(2):
                for cc in range(2):
                    at = (yy * 2 + cc) * rows
                    part[b, yy, cc, :, k * bands:(k + 1) * bands] = value[at:at + rows]

        project_block(layout, beta_k_ref, info_ref, g_k_ref, wave, store, b)
        core_copies.append([
            sends.start(part.at[b, yy, 1 - c], core_in.at[b, yy], other_core) for yy in range(2)
        ])
    for b in range(RING):
        for yy in range(2):
            core_copies[b][yy].wait_recv()
            mine[b, yy] = add(part[b, yy, c], core_in[b, yy]).astype(BF16)

    zb_up = sends.start(mine.at[far, :, :, high_left], zb_in.at[0], next_z)
    zb_down = sends.start(mine.at[far, :, :, high_right], zb_in.at[1], last_z)
    y_copies = [sends.start(mine.at[b, 1 - y, :, low], y_in.at[b], other_y) for b in range(RING)]
    zb_up_own = sends.start(mine.at[up, :, :, high_right], zb_in.at[2], next_z)
    zb_down_own = sends.start(mine.at[down, :, :, high_left], zb_in.at[3], last_z)

    load.wait()
    prepare_block(layout, beta_kq, info_ref, g_kq_ref, left, 0)
    prepare_block(layout, beta_kq, info_ref, g_kq_ref, left, 1)
    zb_up.wait_recv()
    zb_mid[0] = add(mine[up, :, :, half:half + bands], zb_in[0]).astype(BF16)
    zb_up_sum = sends.start(zb_mid.at[0], zb_in.at[4], next_z)
    zb_down.wait_recv()
    zb_mid[1] = add(mine[down, :, :, half + bands:], zb_in[1]).astype(BF16)
    zb_down_sum = sends.start(zb_mid.at[1], zb_in.at[5], last_z)

    for b in range(RING):
        y_copies[b].wait_recv()
        y_sum[b] = add(mine[b, y, :, :half], y_in[b]).astype(BF16)
    za_up = sends.start(y_sum.at[far, :, left_cols], za_in.at[0], next_z)
    za_down = sends.start(y_sum.at[far, :, right_cols], za_in.at[1], last_z)
    za_up_own = sends.start(y_sum.at[up, :, right_cols], za_in.at[2], next_z)
    za_down_own = sends.start(y_sum.at[down, :, left_cols], za_in.at[3], last_z)

    prepare_block(layout, beta_kq, info_ref, g_kq_ref, left, 2)
    for copy in (zb_up_own, zb_down_own, zb_up_sum, zb_down_sum):
        copy.wait_recv()
    b_sum[:, :, :bands] = add(mine[z, :, :, half:half + bands], zb_in[4], zb_in[3]).astype(BF16)
    b_sum[:, :, bands:] = add(mine[z, :, :, half + bands:], zb_in[5], zb_in[2]).astype(BF16)
    b_y = sends.start(b_sum.at[1 - y], b_in, other_y)

    za_up.wait_recv()
    za_mid[0] = add(y_sum[up, :, :bands], za_in[0]).astype(BF16)
    za_up_sum = sends.start(za_mid.at[0], za_in.at[4], next_z)
    za_down.wait_recv()
    za_mid[1] = add(y_sum[down, :, bands:], za_in[1]).astype(BF16)
    za_down_sum = sends.start(za_mid.at[1], za_in.at[5], last_z)

    prepare_block(layout, beta_kq, info_ref, g_kq_ref, left, 3)

    def couple(value):
        return jnp.dot(
            coupling_ref[...], value, precision=lax.Precision.HIGHEST, preferred_element_type=F32
        ).astype(BF16)

    b_y.wait_recv()
    coupled[z, y, c, :, half:] = couple(add(b_sum[y], b_in[...]))
    own = coupled.at[z, y, c, :, high]
    gb_y = sends.start(own, own, other_y)
    for copy in (za_up_own, za_down_own, za_up_sum, za_down_sum):
        copy.wait_recv()
    coupled[z, y, c, :, :bands] = couple(add(y_sum[z, :, :bands], za_in[4], za_in[3]))
    coupled[z, y, c, :, bands:half] = couple(add(y_sum[z, :, bands:], za_in[5], za_in[2]))

    own = coupled.at[z, y, c, :, low]
    ga_up = sends.start(own, own, next_z)
    ga_down = sends.start(own, own, last_z)
    ga_y = [sends.start(own, own, other_y)]
    gc = [sends.start(coupled.at[z, y, c], coupled.at[z, y, c], other_core)]
    gb_y.wait_recv()
    pair = coupled.at[z, :, c, :, high]
    gb_up = sends.start(pair, pair, next_z)
    gb_down = sends.start(pair, pair, last_z)

    def forward(ref, device):
        return sends.start(ref, ref, device)

    ga_up.wait_recv()
    from_down_a = coupled.at[down, y, c, :, low]
    ga_up2 = forward(coupled.at[down, y, c, :, left_cols], next_z)
    ga_y.append(forward(from_down_a, other_y))
    ga_down.wait_recv()
    from_up_a = coupled.at[up, y, c, :, low]
    ga_down2 = forward(coupled.at[up, y, c, :, right_cols], last_z)
    ga_y.append(forward(from_up_a, other_y))
    ga_y[0].wait_recv()
    gc.append(forward(coupled.at[z, 1 - y, c], other_core))

    gb_up.wait_recv()
    gb_up2 = forward(coupled.at[down, :, c, :, high_left], next_z)
    gc_down = forward(coupled.at[down, :, c, :, high], other_core)
    gb_down.wait_recv()
    gb_down2 = forward(coupled.at[up, :, c, :, high_right], last_z)
    gc_up = forward(coupled.at[up, :, c, :, high], other_core)

    def back(b, first):
        parts = back_block(left, b, coupled[b].reshape(layout.block, 2 * half))
        for k in range(2):
            total[k] = parts[k] if first else total[k] + parts[k]

    for copy in gc:
        copy.wait_recv()
    back(z, True)

    ga_up2.wait_recv()
    ga_down2.wait_recv()
    ga_y.append(forward(coupled.at[far, y, c, :, low], other_y))
    ga_y[1].wait_recv()
    gc_down_a = forward(coupled.at[down, :, c, :, low], other_core)
    ga_y[2].wait_recv()
    gc_up_a = forward(coupled.at[up, :, c, :, low], other_core)
    gc_down.wait_recv()
    gc_down_a.wait_recv()
    back(down, False)
    gb_up2.wait_recv()
    gb_down2.wait_recv()
    gc_far = forward(coupled.at[far, :, c, :, high], other_core)
    ga_y[3].wait_recv()
    gc_far_a = forward(coupled.at[far, :, c, :, low], other_core)
    gc_up.wait_recv()
    gc_up_a.wait_recv()
    back(up, False)
    gc_far.wait_recv()
    gc_far_a.wait_recv()
    parts = back_block(left, far, coupled[far].reshape(layout.block, 2 * half))
    for k in range(2):
        out_ref[k] = (total[k] + parts[k]).astype(BF16)
    sends.finish()


COPIES = 64


def fused(layout, arrived, slots, beta_k, beta_kq, info, g_k, g_kq, coupling):
    rows, width = slots.shape[1], arrived.shape[1]
    bands = width // 2
    r = layout.rows
    vmem = pl.BlockSpec(memory_space=pltpu.VMEM)

    def buffer(*shape, dtype=BF16):
        return pltpu.VMEM(shape, dtype)

    return pl.pallas_call(
        functools.partial(fused_kernel, layout),
        in_specs=[vmem] * 7 + [pl.BlockSpec(memory_space=pl.ANY)],
        out_specs=vmem,
        out_shape=jax.ShapeDtypeStruct((2, rows, bands), BF16),
        scratch_shapes=[
            buffer(rows, width),
            buffer(RING, 2, 2, r, 2 * width),
            buffer(RING, 2, r, 2 * width),
            buffer(RING, 2, r, 2 * width),
            buffer(RING, r, width),
            buffer(RING, r, width),
            buffer(6, r, bands),
            buffer(2, r, bands),
            buffer(6, 2, r, bands),
            buffer(2, 2, r, bands),
            buffer(2, r, width),
            buffer(r, width),
            buffer(RING, 2, 2, r, 2 * width),
            buffer(RING, 4, rows, layout.block),
            buffer(2, rows, bands, dtype=F32),
            pltpu.VMEM(beta_kq.shape, BF16),
            pltpu.SemaphoreType.DMA((COPIES,)),
            pltpu.SemaphoreType.DMA((COPIES,)),
            pltpu.SemaphoreType.DMA,
        ],
        compiler_params=params(collective_id=0, has_side_effects=True),
    )(arrived, slots, beta_k, info, g_k, g_kq, coupling, beta_kq)


def pad_rows(layout, values, fill):
    k = values.shape[0]
    parts = values.reshape(k, layout.groups, layout.used)
    parts = jnp.pad(parts, ((0, 0), (0, 0), (0, layout.rows - layout.used)), constant_values=fill)
    parts = parts.reshape(k, layout.blocks, layout.block)
    parts = jnp.pad(parts, ((0, 0), (0, 0), (0, layout.padded - layout.block)), constant_values=fill)
    return parts.reshape(k, layout.blocks * layout.padded)


def block_coupling(layout, dmat, atoms):
    mine = lax.dynamic_slice_in_dim(atoms, lax.axis_index("ga") * layout.per_shard, layout.per_shard)
    blocks = jnp.take(dmat, mine, axis=0)
    eye = jnp.eye(layout.per_shard, dtype=F32)
    full = (blocks[:, :, None, :] * eye[:, None, :, None]).reshape(layout.used, layout.used)
    extra = layout.rows - layout.used
    return jnp.pad(full, ((0, extra), (0, extra)))


def on_device(psi_k, beta_k, beta_kq, g_k, g_kq, send_index, recv_index, dmat, displaced, mode):
    groups = lax.axis_size("ga")
    total = beta_k.shape[2]
    rows = beta_k.shape[1]
    per_atom = dmat.shape[1]
    layout = Layout(groups, displaced.shape[0], per_atom, total)

    packed = pack_rows(send_index.reshape(1, -1), psi_k)
    arrived = lax.all_to_all(packed, "ga", split_axis=0, concat_axis=0, tiled=True)

    rank = jnp.sum((displaced[None, :] < displaced[:, None]).astype(jnp.int32), axis=1)
    place = rank[None, :] == jnp.arange(displaced.shape[0], dtype=jnp.int32)[:, None]
    atoms = jnp.sum(jnp.where(place, displaced[None, :], 0), axis=1)
    moves = jnp.sum(jnp.where(place[None], mode[:, None, :], 0.0), axis=2)
    steps = jnp.tile(jnp.arange(per_atom, dtype=F32), displaced.shape[0])
    source = jnp.repeat(atoms.astype(F32) * per_atom, per_atom) + steps
    source = pad_rows(layout, source[None], -1.0)
    weights = pad_rows(layout, jnp.repeat(moves, per_atom, axis=1), 0.0)
    filler = jnp.zeros((8 - 1 - weights.shape[0], source.shape[1]), F32)
    info = jnp.concatenate([source, weights, filler], axis=0)
    coupling = block_coupling(layout, dmat, atoms)
    run = fused if groups == RING * CORE_Y else separate_steps
    return run(
        layout, arrived, recv_index.reshape(1, -1), jnp.transpose(beta_k, (0, 2, 1)),
        jnp.transpose(beta_kq, (0, 2, 1)), info, g_k, g_kq, coupling,
    )


def solution(mesh):
    in_specs = (
        P(None, "ga", None),
        P(None, "ga", None),
        P(None, "ga", None),
        P(None, "ga"),
        P(None, "ga"),
        P("ga", None, None),
        P("ga"),
        P(),
        P("pert"),
        P(None, "pert"),
    )
    out_specs = P("pert", "ga", None)
    return jax.shard_map(
        on_device, mesh=mesh, in_specs=in_specs, out_specs=out_specs, check_vma=False
    )
```

```python
import functools

import jax
import jax.numpy as jnp
import numpy as np
from jax import lax
from jax.experimental import pallas as pl
from jax.experimental.pallas import tpu as pltpu
from jax.sharding import PartitionSpec as P

LANES = 128
RING = 4
CORE_Y = 4
BF16 = jnp.bfloat16
F32 = jnp.float32
VMEM_LIMIT = 56 * 1024 * 1024


def round_up(value, step):
    return -(-value // step) * step


def dot(a, b):
    return jnp.dot(a, b, preferred_element_type=F32)


def dot_t(a, b):
    return lax.dot_general(a, b, (((0,), (0,)), ((), ())), preferred_element_type=F32)


def pack_kernel(slot_ref, psi_ref, out_ref):
    rows = psi_ref.shape[1]
    bands = psi_ref.shape[2]
    slots = slot_ref.shape[1]
    pick = (lax.broadcasted_iota(jnp.int32, (rows, slots), 0) == slot_ref[...]).astype(BF16)
    for part in range(2):
        out_ref[:, part * bands:(part + 1) * bands] = dot_t(pick, psi_ref[part]).astype(BF16)


def pack_rows(slots, psi_k):
    return pl.pallas_call(
        pack_kernel,
        out_shape=jax.ShapeDtypeStruct((slots.shape[1], 2 * psi_k.shape[2]), BF16),
        compiler_params=pltpu.CompilerParams(vmem_limit_bytes=VMEM_LIMIT),
    )(slots, psi_k)


class Layout:
    def __init__(self, groups, atoms, per_atom, total):
        self.groups = groups
        self.blocks = groups // CORE_Y
        self.gang = CORE_Y
        if self.blocks != RING:
            self.blocks = RING
            self.gang = groups // RING
        self.per_shard = atoms // groups
        self.per_atom = per_atom
        self.used = self.per_shard * per_atom
        self.rows = round_up(self.used, 16)
        self.block = self.gang * self.rows
        self.padded = round_up(self.block, LANES)
        self.total = total
        slack = total - atoms * per_atom
        self.window = min(total, round_up(self.gang * self.used + slack + 16, LANES))
        self.starts = [
            min(b * self.gang * self.used // 16 * 16, total - self.window) for b in range(self.blocks)
        ]


def columns_of(layout, info_ref, b):
    wide = info_ref[:, b * layout.padded:(b + 1) * layout.padded]
    return jnp.transpose(wide)[: layout.block]


def select(layout, beta_ref, info, b):
    start = layout.starts[b]
    ids = lax.broadcasted_iota(jnp.int32, (layout.block, layout.window), 1) + start
    pick = (ids == info[:, 0:1].astype(jnp.int32)).astype(BF16)
    rows = pl.ds(start, layout.window)
    return dot(pick, beta_ref[0, rows, :]), dot(pick, beta_ref[1, rows, :])


def row_scale(g_ref, info):
    total = info[:, 1:2] * g_ref[0:1, :]
    for x in range(1, g_ref.shape[0]):
        total = total + info[:, x + 1:x + 2] * g_ref[x:x + 1, :]
    return total


def regroup(arrived_ref, slot_ref, wave):
    slots, rows = arrived_ref.shape[0], wave.shape[0]
    pick = (lax.broadcasted_iota(jnp.int32, (slots, rows), 0) == slot_ref[...]).astype(BF16)
    wave[...] = dot_t(pick, arrived_ref[...]).astype(BF16)


def selected_terms(layout, beta_ref, info, g_ref, b):
    real, imag = select(layout, beta_ref, info, b)
    scale = row_scale(g_ref, info)
    return real, imag, scale * imag, scale * real


def project_block(terms, stacked, store):
    bands = stacked.shape[1] // 2
    x = dot(terms[0], stacked)
    y = dot(terms[1], stacked)
    store(0, (x[:, :bands] + y[:, bands:]).astype(BF16))
    store(1, (x[:, bands:] - y[:, :bands]).astype(BF16))
    x = dot(terms[2], stacked)
    y = dot(terms[3], stacked)
    store(2, (x[:, :bands] - y[:, bands:]).astype(BF16))
    store(3, (x[:, bands:] + y[:, :bands]).astype(BF16))


def prepare_block(layout, beta_ref, info, g_ref, left_ref, b):
    real, imag, slope_real, slope_imag = selected_terms(layout, beta_ref, info, g_ref, b)
    for k, term in enumerate((slope_real, -slope_imag, real, imag)):
        left_ref[b, k] = term.astype(BF16).T


def back_block(left_ref, b, coupled):
    width = coupled.shape[1] // 2
    bands = width // 2
    first, second = coupled[:, :width], coupled[:, width:]
    x = dot(left_ref[b, 0], first) + dot(left_ref[b, 2], second)
    y = dot(left_ref[b, 1], first) + dot(left_ref[b, 3], second)
    return x[:, :bands] - y[:, bands:], x[:, bands:] + y[:, :bands]


def project_kernel(layout, arrived_ref, slot_ref, beta_ref, info_ref, g_ref, out_ref, wave):
    regroup(arrived_ref, slot_ref, wave)
    bands = wave.shape[1] // 2
    for b in range(layout.blocks):

        def store(k, value, b=b):
            out_ref[b * layout.block:(b + 1) * layout.block, k * bands:(k + 1) * bands] = value

        info = columns_of(layout, info_ref, b)
        terms = [term.astype(BF16) for term in selected_terms(layout, beta_ref, info, g_ref, b)]
        project_block(terms, wave[...], store)


def finish_kernel(layout, beta_ref, info_ref, g_ref, coupled_ref, out_ref, left, total):
    for b in range(layout.blocks):
        prepare_block(layout, beta_ref, columns_of(layout, info_ref, b), g_ref, left, b)
        parts = back_block(left, b, coupled_ref[b * layout.block:(b + 1) * layout.block, :])
        for k in range(2):
            total[k] = parts[k] if b == 0 else total[k] + parts[k]
    out_ref[...] = total[...].astype(BF16)


def params(**extra):
    return pltpu.CompilerParams(vmem_limit_bytes=VMEM_LIMIT, **extra)


def separate_steps(layout, arrived, slots, beta_k, beta_kq, info, g_k, g_kq, coupling):
    rows, width = slots.shape[1], arrived.shape[1]
    terms = pl.pallas_call(
        functools.partial(project_kernel, layout),
        out_shape=jax.ShapeDtypeStruct((layout.groups * layout.rows, 2 * width), BF16),
        scratch_shapes=[pltpu.VMEM((rows, width), BF16)],
        compiler_params=params(),
    )(arrived, slots, beta_k, info, g_k)
    shard = lax.psum_scatter(terms.astype(F32), "ga", scatter_dimension=0, tiled=True)
    mixed = jnp.dot(
        coupling, shard, precision=lax.Precision.HIGHEST, preferred_element_type=F32
    ).astype(BF16)
    coupled = lax.all_gather(mixed, "ga", axis=0, tiled=True)
    return pl.pallas_call(
        functools.partial(finish_kernel, layout),
        out_shape=jax.ShapeDtypeStruct((2, rows, width // 2), BF16),
        scratch_shapes=[
            pltpu.VMEM((layout.blocks, 4, rows, layout.block), BF16),
            pltpu.VMEM((2, rows, width // 2), F32),
        ],
        compiler_params=params(),
    )(beta_kq, info, g_kq, coupled)


class Sends:
    def __init__(self, send_sem, recv_sem):
        self.send_sem, self.recv_sem = send_sem, recv_sem
        self.started = []

    def start(self, source, target, device):
        k = len(self.started)
        copy = pltpu.make_async_remote_copy(
            src_ref=source,
            dst_ref=target,
            send_sem=self.send_sem.at[k],
            recv_sem=self.recv_sem.at[k],
            device_id={"ga": device},
            device_id_type=pl.DeviceIdType.MESH,
        )
        copy.start()
        self.started.append(copy)
        return copy

    def finish(self):
        for copy in self.started:
            copy.wait_send()


def exact_dot(a, b):
    return jnp.dot(a, b, precision=lax.Precision.HIGHEST, preferred_element_type=F32)


def slot_row(send_ref):
    receivers, cap = send_ref.shape
    column = lax.broadcasted_iota(jnp.int32, (cap, receivers * cap), 1)
    inner = lax.broadcasted_iota(jnp.int32, (cap, receivers * cap), 0)
    wide = exact_dot(send_ref[...].astype(F32), (column % cap == inner).astype(F32))
    column = lax.broadcasted_iota(jnp.int32, wide.shape, 1)
    outer = lax.broadcasted_iota(jnp.int32, wide.shape, 0)
    return jnp.sum(jnp.where(column // cap == outer, wide, 0.0), axis=0, keepdims=True).astype(jnp.int32)


def sorted_info(layout, displaced_ref, mode_ref, table_ref, values, info):
    parts = mode_ref.shape[0]
    values[...] = jnp.zeros_like(values)
    values[0:1, :] = displaced_ref[...].astype(F32)
    values[1:1 + parts, :] = mode_ref[...]
    by_atom = jnp.transpose(values[...])
    smaller = (by_atom[:, 0:1] < values[0:1, :]).astype(F32)
    rank = jnp.sum(smaller, axis=0, keepdims=True)
    lane = lax.broadcasted_iota(jnp.int32, (layout.block, values.shape[0]), 1)
    for b in range(layout.blocks):
        place = columns_of(layout, table_ref, b)
        found = exact_dot((place[:, 0:1] == rank).astype(F32), by_atom)
        source = jnp.where(place[:, 0:1] < 0, -1.0, found * layout.per_atom + place[:, 1:2])
        info[b] = jnp.where(lane == 0, source, jnp.where(lane == 7, found[:, 0:1], found))


def coupling_matrix(layout, dmat_ref, atom, proj, spread_ref, same_ref):
    lanes = lax.broadcasted_iota(jnp.int32, (layout.rows, dmat_ref.shape[2]), 1)
    pick = (lanes == atom.astype(jnp.int32)).astype(F32)
    rows = jnp.zeros((layout.rows, layout.per_atom), F32)
    for i in range(layout.per_atom):
        found = lax.dot_general(
            pick, dmat_ref[i], (((1,), (1,)), ((), ())),
            precision=lax.Precision.HIGHEST, preferred_element_type=F32,
        )
        rows = rows + jnp.where(proj == i, found, 0.0)
    return exact_dot(rows, spread_ref[...]) * same_ref[...]


def fused_kernel(
    layout, psi_ref, send_ref, slot_ref, displaced_ref, mode_ref, table_ref, g_k_ref, g_kq_ref, dmat_ref,
    proj_ref, spread_ref, same_ref, beta_k_hbm, beta_kq_hbm,
    out_ref, wave, part, core_in, mine, y_in, y_sum, za_in, za_mid, zb_in, zb_mid, b_sum, b_in,
    coupled, left, total, beta_kq, beta_k, packed, arrived, terms, values, info, send_sem, recv_sem, load_sem,
):
    me = lax.axis_index("ga")
    n = layout.groups
    c, y, z = me % 2, (me // 2) % 2, me // 4

    def index(zz, yy, cc):
        return (zz * 2 + yy) * 2 + cc

    up, down, far = (z + 1) % RING, (z + RING - 1) % RING, (z + 2) % RING
    other_core, other_y = index(z, y, 1 - c), index(z, 1 - y, c)
    next_z, last_z = index(up, y, c), index(down, y, c)
    load_k = pltpu.make_async_copy(beta_k_hbm, beta_k, load_sem.at[0])
    load_k.start()
    load = pltpu.make_async_copy(beta_kq_hbm, beta_kq, load_sem.at[1])
    load.start()

    barrier = pltpu.get_barrier_semaphore()
    for step in range(1, n):
        pl.semaphore_signal(
            barrier, inc=1, device_id={"ga": (me + step) % n}, device_id_type=pl.DeviceIdType.MESH
        )
    rows_here, slots = psi_ref.shape[1], n * send_ref.shape[1]
    cap = send_ref.shape[1]
    pick = (lax.broadcasted_iota(jnp.int32, (rows_here, slots), 0) == slot_row(send_ref)).astype(BF16)
    for k in range(2):
        width = psi_ref.shape[2]
        packed[:, :, k * width:(k + 1) * width] = dot_t(pick, psi_ref[k]).astype(BF16).reshape(n, cap, width)
    pl.semaphore_wait(barrier, n - 1)

    sends = Sends(send_sem, recv_sem)
    rows = layout.rows
    bands = wave.shape[1] // 2
    half = 2 * bands
    low, high = pl.ds(0, half), pl.ds(half, half)
    left_cols, right_cols = pl.ds(0, bands), pl.ds(bands, bands)
    high_left, high_right = pl.ds(half, bands), pl.ds(half + bands, bands)

    def add(first, *others):
        value = first.astype(F32)
        for other in others:
            value = value + other.astype(F32)
        return value

    psi_copies = [
        sends.start(packed.at[(me + step) % n], arrived.at[me], (me + step) % n) for step in far_first(n)
    ]
    arrived[me] = packed[me]
    sorted_info(layout, displaced_ref, mode_ref, table_ref, values, info)
    load_k.wait()
    for b in range(RING):
        for k, term in enumerate(selected_terms(layout, beta_k, info[b], g_k_ref, b)):
            terms[b, k] = term.astype(BF16)
    load.wait()
    prepare_block(layout, beta_kq, info[0], g_kq_ref, left, 0)
    for copy in psi_copies:
        copy.wait_recv()

    pick = (lax.broadcasted_iota(jnp.int32, (slots, rows_here), 0) == slot_ref[...]).astype(BF16)
    wave[...] = dot_t(pick, arrived[...].reshape(slots, 2 * bands)).astype(BF16)
    core_copies = []
    for b in range(RING):

        def store(k, value, b=b):
            for yy in range(2):
                for cc in range(2):
                    at = (yy * 2 + cc) * rows
                    part[b, yy, cc, :, k * bands:(k + 1) * bands] = value[at:at + rows]

        project_block([terms[b, k] for k in range(4)], wave[...], store)
        core_copies.append([
            sends.start(part.at[b, yy, 1 - c], core_in.at[b, yy], other_core) for yy in range(2)
        ])
    for b in range(RING):
        for yy in range(2):
            core_copies[b][yy].wait_recv()
            mine[b, yy] = add(part[b, yy, c], core_in[b, yy]).astype(BF16)

    zb_up = sends.start(mine.at[far, :, :, high_left], zb_in.at[0], next_z)
    zb_down = sends.start(mine.at[far, :, :, high_right], zb_in.at[1], last_z)
    y_copies = [sends.start(mine.at[b, 1 - y, :, low], y_in.at[b], other_y) for b in range(RING)]
    zb_up_own = sends.start(mine.at[up, :, :, high_right], zb_in.at[2], next_z)
    zb_down_own = sends.start(mine.at[down, :, :, high_left], zb_in.at[3], last_z)

    shard_atom = info[z, pl.ds(pl.multiple_of((y * 2 + c) * rows, 8), rows), 7:8]
    coupling = coupling_matrix(layout, dmat_ref, shard_atom, proj_ref[...], spread_ref, same_ref)
    prepare_block(layout, beta_kq, info[1], g_kq_ref, left, 1)
    zb_up.wait_recv()
    zb_mid[0] = add(mine[up, :, :, half:half + bands], zb_in[0]).astype(BF16)
    zb_up_sum = sends.start(zb_mid.at[0], zb_in.at[4], next_z)
    zb_down.wait_recv()
    zb_mid[1] = add(mine[down, :, :, half + bands:], zb_in[1]).astype(BF16)
    zb_down_sum = sends.start(zb_mid.at[1], zb_in.at[5], last_z)

    for b in range(RING):
        y_copies[b].wait_recv()
        y_sum[b] = add(mine[b, y, :, :half], y_in[b]).astype(BF16)
    za_up = sends.start(y_sum.at[far, :, left_cols], za_in.at[0], next_z)
    za_down = sends.start(y_sum.at[far, :, right_cols], za_in.at[1], last_z)
    za_up_own = sends.start(y_sum.at[up, :, right_cols], za_in.at[2], next_z)
    za_down_own = sends.start(y_sum.at[down, :, left_cols], za_in.at[3], last_z)

    prepare_block(layout, beta_kq, info[2], g_kq_ref, left, 2)
    for copy in (zb_up_own, zb_down_own, zb_up_sum, zb_down_sum):
        copy.wait_recv()
    b_sum[:, :, :bands] = add(mine[z, :, :, half:half + bands], zb_in[4], zb_in[3]).astype(BF16)
    b_sum[:, :, bands:] = add(mine[z, :, :, half + bands:], zb_in[5], zb_in[2]).astype(BF16)
    b_y = sends.start(b_sum.at[1 - y], b_in, other_y)

    za_up.wait_recv()
    za_mid[0] = add(y_sum[up, :, :bands], za_in[0]).astype(BF16)
    za_up_sum = sends.start(za_mid.at[0], za_in.at[4], next_z)
    za_down.wait_recv()
    za_mid[1] = add(y_sum[down, :, bands:], za_in[1]).astype(BF16)
    za_down_sum = sends.start(za_mid.at[1], za_in.at[5], last_z)

    prepare_block(layout, beta_kq, info[3], g_kq_ref, left, 3)

    def couple(value):
        return exact_dot(coupling, value).astype(BF16)

    b_y.wait_recv()
    coupled[z, y, c, :, half:] = couple(add(b_sum[y], b_in[...]))
    own = coupled.at[z, y, c, :, high]
    gb_y = sends.start(own, own, other_y)
    for copy in (za_up_own, za_down_own, za_up_sum, za_down_sum):
        copy.wait_recv()
    coupled[z, y, c, :, :bands] = couple(add(y_sum[z, :, :bands], za_in[4], za_in[3]))
    coupled[z, y, c, :, bands:half] = couple(add(y_sum[z, :, bands:], za_in[5], za_in[2]))

    own = coupled.at[z, y, c, :, low]
    ga_up = sends.start(own, own, next_z)
    ga_down = sends.start(own, own, last_z)
    ga_y = [sends.start(own, own, other_y)]
    gc = [sends.start(coupled.at[z, y, c], coupled.at[z, y, c], other_core)]
    gb_y.wait_recv()
    pair = coupled.at[z, :, c, :, high]
    gb_up = sends.start(pair, pair, next_z)
    gb_down = sends.start(pair, pair, last_z)

    def forward(ref, device):
        return sends.start(ref, ref, device)

    ga_up.wait_recv()
    from_down_a = coupled.at[down, y, c, :, low]
    ga_up2 = forward(coupled.at[down, y, c, :, left_cols], next_z)
    ga_y.append(forward(from_down_a, other_y))
    ga_down.wait_recv()
    from_up_a = coupled.at[up, y, c, :, low]
    ga_down2 = forward(coupled.at[up, y, c, :, right_cols], last_z)
    ga_y.append(forward(from_up_a, other_y))
    ga_y[0].wait_recv()
    gc.append(forward(coupled.at[z, 1 - y, c], other_core))

    gb_up.wait_recv()
    gb_up2 = forward(coupled.at[down, :, c, :, high_left], next_z)
    gc_down = forward(coupled.at[down, :, c, :, high], other_core)
    gb_down.wait_recv()
    gb_down2 = forward(coupled.at[up, :, c, :, high_right], last_z)
    gc_up = forward(coupled.at[up, :, c, :, high], other_core)

    def back(b, first):
        parts = back_block(left, b, coupled[b].reshape(layout.block, 2 * half))
        for k in range(2):
            total[k] = parts[k] if first else total[k] + parts[k]

    for copy in gc:
        copy.wait_recv()
    back(z, True)

    ga_up2.wait_recv()
    ga_down2.wait_recv()
    ga_y.append(forward(coupled.at[far, y, c, :, low], other_y))
    ga_y[1].wait_recv()
    gc_down_a = forward(coupled.at[down, :, c, :, low], other_core)
    ga_y[2].wait_recv()
    gc_up_a = forward(coupled.at[up, :, c, :, low], other_core)
    gc_down.wait_recv()
    gc_down_a.wait_recv()
    back(down, False)
    gb_up2.wait_recv()
    gb_down2.wait_recv()
    gc_far = forward(coupled.at[far, :, c, :, high], other_core)
    ga_y[3].wait_recv()
    gc_far_a = forward(coupled.at[far, :, c, :, low], other_core)
    gc_up.wait_recv()
    gc_up_a.wait_recv()
    back(up, False)
    gc_far.wait_recv()
    gc_far_a.wait_recv()
    parts = back_block(left, far, coupled[far].reshape(layout.block, 2 * half))
    for k in range(2):
        out_ref[k] = (total[k] + parts[k]).astype(BF16)
    sends.finish()


COPIES = 80


def far_first(n):
    return sorted(range(1, n), key=lambda step: -min(step, n - step))


def tables(layout):
    row = np.arange(layout.rows)
    valid = row < layout.used
    slot = np.where(valid, row // layout.per_atom, 0)
    proj = np.where(valid, row % layout.per_atom, -1)
    table = np.zeros((8, layout.blocks, layout.padded), np.float32)
    table[0] = -1.0
    for b in range(layout.blocks):
        for k in range(layout.gang):
            at = slice(k * layout.rows, (k + 1) * layout.rows)
            table[0, b, at] = np.where(valid, (b * layout.gang + k) * layout.per_shard + slot, -1)
            table[1, b, at] = np.where(valid, proj, 0)
    spread = (np.arange(layout.per_atom)[:, None] == proj[None]).astype(np.float32)
    same = (slot[:, None] == slot[None]) & valid[:, None] & valid[None]
    return (
        table.reshape(8, -1),
        proj[:, None].astype(np.int32),
        spread,
        same.astype(np.float32),
    )


def fused(layout, psi_k, send_index, recv_index, beta_k, beta_kq, displaced, mode, g_k, g_kq, dmat):
    rows, bands = psi_k.shape[1:]
    width = 2 * bands
    cap = send_index.shape[2]
    table, proj, spread, same = (jnp.asarray(value) for value in tables(layout))
    r = layout.rows
    vmem = pl.BlockSpec(memory_space=pltpu.VMEM)

    def buffer(*shape, dtype=BF16):
        return pltpu.VMEM(shape, dtype)

    return pl.pallas_call(
        functools.partial(fused_kernel, layout),
        in_specs=[vmem] * 12 + [pl.BlockSpec(memory_space=pl.ANY)] * 2,
        out_specs=vmem,
        out_shape=jax.ShapeDtypeStruct((2, rows, bands), BF16),
        scratch_shapes=[
            buffer(rows, width),
            buffer(RING, 2, 2, r, 2 * width),
            buffer(RING, 2, r, 2 * width),
            buffer(RING, 2, r, 2 * width),
            buffer(RING, r, width),
            buffer(RING, r, width),
            buffer(6, r, bands),
            buffer(2, r, bands),
            buffer(6, 2, r, bands),
            buffer(2, 2, r, bands),
            buffer(2, r, width),
            buffer(r, width),
            buffer(RING, 2, 2, r, 2 * width),
            buffer(RING, 4, rows, layout.block),
            buffer(2, rows, bands, dtype=F32),
            pltpu.VMEM(beta_kq.shape, BF16),
            pltpu.VMEM(beta_k.shape, BF16),
            buffer(layout.groups, cap, width),
            buffer(layout.groups, cap, width),
            buffer(RING, 4, layout.block, rows),
            buffer(8, displaced.shape[0], dtype=F32),
            buffer(RING, layout.block, 8, dtype=F32),
            pltpu.SemaphoreType.DMA((COPIES,)),
            pltpu.SemaphoreType.DMA((COPIES,)),
            pltpu.SemaphoreType.DMA((2,)),
        ],
        compiler_params=params(collective_id=0, has_side_effects=True),
    )(
        psi_k, send_index[0], recv_index.reshape(1, -1), displaced.reshape(1, -1), mode, table, g_k, g_kq,
        jnp.transpose(dmat, (1, 2, 0)), proj, spread, same, beta_k, beta_kq,
    )


def pad_rows(layout, values, fill):
    k = values.shape[0]
    parts = values.reshape(k, layout.groups, layout.used)
    parts = jnp.pad(parts, ((0, 0), (0, 0), (0, layout.rows - layout.used)), constant_values=fill)
    parts = parts.reshape(k, layout.blocks, layout.block)
    parts = jnp.pad(parts, ((0, 0), (0, 0), (0, layout.padded - layout.block)), constant_values=fill)
    return parts.reshape(k, layout.blocks * layout.padded)


def block_coupling(layout, dmat, atoms):
    mine = lax.dynamic_slice_in_dim(atoms, lax.axis_index("ga") * layout.per_shard, layout.per_shard)
    blocks = jnp.take(dmat, mine, axis=0)
    eye = jnp.eye(layout.per_shard, dtype=F32)
    full = (blocks[:, :, None, :] * eye[:, None, :, None]).reshape(layout.used, layout.used)
    extra = layout.rows - layout.used
    return jnp.pad(full, ((0, extra), (0, extra)))


def on_device(psi_k, beta_k, beta_kq, g_k, g_kq, send_index, recv_index, dmat, displaced, mode):
    groups = lax.axis_size("ga")
    total = beta_k.shape[2]
    rows = beta_k.shape[1]
    per_atom = dmat.shape[1]
    layout = Layout(groups, displaced.shape[0], per_atom, total)

    beta_k, beta_kq = jnp.transpose(beta_k, (0, 2, 1)), jnp.transpose(beta_kq, (0, 2, 1))
    if groups == RING * CORE_Y:
        return fused(layout, psi_k, send_index, recv_index, beta_k, beta_kq, displaced, mode, g_k, g_kq, dmat)

    packed = pack_rows(send_index.reshape(1, -1), psi_k)
    arrived = lax.all_to_all(packed, "ga", split_axis=0, concat_axis=0, tiled=True)

    rank = jnp.sum((displaced[None, :] < displaced[:, None]).astype(jnp.int32), axis=1)
    place = rank[None, :] == jnp.arange(displaced.shape[0], dtype=jnp.int32)[:, None]
    atoms = jnp.sum(jnp.where(place, displaced[None, :], 0), axis=1)
    moves = jnp.sum(jnp.where(place[None], mode[:, None, :], 0.0), axis=2)
    steps = jnp.tile(jnp.arange(per_atom, dtype=F32), displaced.shape[0])
    source = jnp.repeat(atoms.astype(F32) * per_atom, per_atom) + steps
    source = pad_rows(layout, source[None], -1.0)
    weights = pad_rows(layout, jnp.repeat(moves, per_atom, axis=1), 0.0)
    filler = jnp.zeros((8 - 1 - weights.shape[0], source.shape[1]), F32)
    info = jnp.concatenate([source, weights, filler], axis=0)
    coupling = block_coupling(layout, dmat, atoms)
    return separate_steps(
        layout, arrived, recv_index.reshape(1, -1), beta_k, beta_kq, info, g_k, g_kq, coupling
    )


def solution(mesh):
    in_specs = (
        P(None, "ga", None),
        P(None, "ga", None),
        P(None, "ga", None),
        P(None, "ga"),
        P(None, "ga"),
        P("ga", None, None),
        P("ga"),
        P(),
        P("pert"),
        P(None, "pert"),
    )
    out_specs = P("pert", "ga", None)
    return jax.shard_map(
        on_device, mesh=mesh, in_specs=in_specs, out_specs=out_specs, check_vma=False
    )
```

```python
import functools

import jax
import jax.numpy as jnp
import numpy as np
from jax import lax
from jax.experimental import pallas as pl
from jax.experimental.pallas import tpu as pltpu
from jax.sharding import PartitionSpec as P

LANES = 128
RING = 4
CORE_Y = 4
BF16 = jnp.bfloat16
F32 = jnp.float32
VMEM_LIMIT = 56 * 1024 * 1024


def round_up(value, step):
    return -(-value // step) * step


def dot(a, b):
    return jnp.dot(a, b, preferred_element_type=F32)


def dot_t(a, b):
    return lax.dot_general(a, b, (((0,), (0,)), ((), ())), preferred_element_type=F32)


def pack_kernel(slot_ref, psi_ref, out_ref):
    rows = psi_ref.shape[1]
    bands = psi_ref.shape[2]
    slots = slot_ref.shape[1]
    pick = (lax.broadcasted_iota(jnp.int32, (rows, slots), 0) == slot_ref[...]).astype(BF16)
    for part in range(2):
        out_ref[:, part * bands:(part + 1) * bands] = dot_t(pick, psi_ref[part]).astype(BF16)


def pack_rows(slots, psi_k):
    return pl.pallas_call(
        pack_kernel,
        out_shape=jax.ShapeDtypeStruct((slots.shape[1], 2 * psi_k.shape[2]), BF16),
        compiler_params=pltpu.CompilerParams(vmem_limit_bytes=VMEM_LIMIT),
    )(slots, psi_k)


class Layout:
    def __init__(self, groups, atoms, per_atom, total):
        self.groups = groups
        self.blocks = groups // CORE_Y
        self.gang = CORE_Y
        if self.blocks != RING:
            self.blocks = RING
            self.gang = groups // RING
        self.per_shard = atoms // groups
        self.per_atom = per_atom
        self.used = self.per_shard * per_atom
        self.rows = round_up(self.used, 16)
        self.block = self.gang * self.rows
        self.padded = round_up(self.block, LANES)
        self.total = total
        slack = total - atoms * per_atom
        self.window = min(total, round_up(self.gang * self.used + slack + 16, LANES))
        self.starts = [
            min(b * self.gang * self.used // 16 * 16, total - self.window) for b in range(self.blocks)
        ]


def columns_of(layout, info_ref, b):
    wide = info_ref[:, b * layout.padded:(b + 1) * layout.padded]
    return jnp.transpose(wide)[: layout.block]


def select(layout, beta_ref, info, b):
    start = layout.starts[b]
    ids = lax.broadcasted_iota(jnp.int32, (layout.block, layout.window), 1) + start
    pick = (ids == info[:, 0:1].astype(jnp.int32)).astype(BF16)
    rows = pl.ds(start, layout.window)
    return dot(pick, beta_ref[0, rows, :]), dot(pick, beta_ref[1, rows, :])


def row_scale(g_ref, info):
    total = info[:, 1:2] * g_ref[0:1, :]
    for x in range(1, g_ref.shape[0]):
        total = total + info[:, x + 1:x + 2] * g_ref[x:x + 1, :]
    return total


def regroup(arrived_ref, slot_ref, wave):
    slots, rows = arrived_ref.shape[0], wave.shape[0]
    pick = (lax.broadcasted_iota(jnp.int32, (slots, rows), 0) == slot_ref[...]).astype(BF16)
    wave[...] = dot_t(pick, arrived_ref[...]).astype(BF16)


def selected_terms(layout, beta_ref, info, g_ref, b):
    real, imag = select(layout, beta_ref, info, b)
    scale = row_scale(g_ref, info)
    return real, imag, scale * imag, scale * real


def project_block(terms, stacked, store):
    bands = stacked.shape[1] // 2
    x = dot(terms[0], stacked)
    y = dot(terms[1], stacked)
    store(0, (x[:, :bands] + y[:, bands:]).astype(BF16))
    store(1, (x[:, bands:] - y[:, :bands]).astype(BF16))
    x = dot(terms[2], stacked)
    y = dot(terms[3], stacked)
    store(2, (x[:, :bands] - y[:, bands:]).astype(BF16))
    store(3, (x[:, bands:] + y[:, :bands]).astype(BF16))


def prepare_block(layout, beta_ref, info, g_ref, left_ref, b):
    real, imag, slope_real, slope_imag = selected_terms(layout, beta_ref, info, g_ref, b)
    for k, term in enumerate((slope_real, -slope_imag, real, imag)):
        left_ref[b, k] = term.astype(BF16).T


def back_block(left_ref, b, coupled):
    width = coupled.shape[1] // 2
    bands = width // 2
    first, second = coupled[:, :width], coupled[:, width:]
    x = dot(left_ref[b, 0], first) + dot(left_ref[b, 2], second)
    y = dot(left_ref[b, 1], first) + dot(left_ref[b, 3], second)
    return x[:, :bands] - y[:, bands:], x[:, bands:] + y[:, :bands]


def project_kernel(layout, arrived_ref, slot_ref, beta_ref, info_ref, g_ref, out_ref, wave):
    regroup(arrived_ref, slot_ref, wave)
    bands = wave.shape[1] // 2
    for b in range(layout.blocks):

        def store(k, value, b=b):
            out_ref[b * layout.block:(b + 1) * layout.block, k * bands:(k + 1) * bands] = value

        info = columns_of(layout, info_ref, b)
        terms = [term.astype(BF16) for term in selected_terms(layout, beta_ref, info, g_ref, b)]
        project_block(terms, wave[...], store)


def finish_kernel(layout, beta_ref, info_ref, g_ref, coupled_ref, out_ref, left, total):
    for b in range(layout.blocks):
        prepare_block(layout, beta_ref, columns_of(layout, info_ref, b), g_ref, left, b)
        parts = back_block(left, b, coupled_ref[b * layout.block:(b + 1) * layout.block, :])
        for k in range(2):
            total[k] = parts[k] if b == 0 else total[k] + parts[k]
    out_ref[...] = total[...].astype(BF16)


def params(**extra):
    return pltpu.CompilerParams(vmem_limit_bytes=VMEM_LIMIT, **extra)


def separate_steps(layout, arrived, slots, beta_k, beta_kq, info, g_k, g_kq, coupling):
    rows, width = slots.shape[1], arrived.shape[1]
    terms = pl.pallas_call(
        functools.partial(project_kernel, layout),
        out_shape=jax.ShapeDtypeStruct((layout.groups * layout.rows, 2 * width), BF16),
        scratch_shapes=[pltpu.VMEM((rows, width), BF16)],
        compiler_params=params(),
    )(arrived, slots, beta_k, info, g_k)
    shard = lax.psum_scatter(terms.astype(F32), "ga", scatter_dimension=0, tiled=True)
    mixed = jnp.dot(
        coupling, shard, precision=lax.Precision.HIGHEST, preferred_element_type=F32
    ).astype(BF16)
    coupled = lax.all_gather(mixed, "ga", axis=0, tiled=True)
    return pl.pallas_call(
        functools.partial(finish_kernel, layout),
        out_shape=jax.ShapeDtypeStruct((2, rows, width // 2), BF16),
        scratch_shapes=[
            pltpu.VMEM((layout.blocks, 4, rows, layout.block), BF16),
            pltpu.VMEM((2, rows, width // 2), F32),
        ],
        compiler_params=params(),
    )(beta_kq, info, g_kq, coupled)


class Sends:
    def __init__(self, send_sem, recv_sem):
        self.send_sem, self.recv_sem = send_sem, recv_sem
        self.started = []

    def start(self, source, target, device):
        k = len(self.started)
        copy = pltpu.make_async_remote_copy(
            src_ref=source,
            dst_ref=target,
            send_sem=self.send_sem.at[k],
            recv_sem=self.recv_sem.at[k],
            device_id={"ga": device},
            device_id_type=pl.DeviceIdType.MESH,
        )
        copy.start()
        self.started.append(copy)
        return copy

    def finish(self):
        for copy in self.started:
            copy.wait_send()


def exact_dot(a, b):
    return jnp.dot(a, b, precision=lax.Precision.HIGHEST, preferred_element_type=F32)


def slot_row(send_ref):
    receivers, cap = send_ref.shape
    column = lax.broadcasted_iota(jnp.int32, (cap, receivers * cap), 1)
    inner = lax.broadcasted_iota(jnp.int32, (cap, receivers * cap), 0)
    wide = exact_dot(send_ref[...].astype(F32), (column % cap == inner).astype(F32))
    column = lax.broadcasted_iota(jnp.int32, wide.shape, 1)
    outer = lax.broadcasted_iota(jnp.int32, wide.shape, 0)
    return jnp.sum(jnp.where(column // cap == outer, wide, 0.0), axis=0, keepdims=True).astype(jnp.int32)


def sorted_info(layout, displaced_ref, mode_ref, table_ref, values, info):
    parts = mode_ref.shape[0]
    values[...] = jnp.zeros_like(values)
    values[0:1, :] = displaced_ref[...].astype(F32)
    values[1:1 + parts, :] = mode_ref[...]
    by_atom = jnp.transpose(values[...])
    smaller = (by_atom[:, 0:1] < values[0:1, :]).astype(F32)
    rank = jnp.sum(smaller, axis=0, keepdims=True)
    lane = lax.broadcasted_iota(jnp.int32, (layout.block, values.shape[0]), 1)
    for b in range(layout.blocks):
        place = columns_of(layout, table_ref, b)
        found = exact_dot((place[:, 0:1] == rank).astype(F32), by_atom)
        source = jnp.where(place[:, 0:1] < 0, -1.0, found * layout.per_atom + place[:, 1:2])
        info[b] = jnp.where(lane == 0, source, jnp.where(lane == 7, found[:, 0:1], found))


def coupling_matrix(layout, dmat_ref, atom, proj, spread_ref, same_ref):
    lanes = lax.broadcasted_iota(jnp.int32, (layout.rows, dmat_ref.shape[2]), 1)
    pick = (lanes == atom.astype(jnp.int32)).astype(F32)
    rows = jnp.zeros((layout.rows, layout.per_atom), F32)
    for i in range(layout.per_atom):
        found = lax.dot_general(
            pick, dmat_ref[i], (((1,), (1,)), ((), ())),
            precision=lax.Precision.HIGHEST, preferred_element_type=F32,
        )
        rows = rows + jnp.where(proj == i, found, 0.0)
    return exact_dot(rows, spread_ref[...]) * same_ref[...]


def fused_kernel(
    layout, psi_ref, send_ref, slot_ref, displaced_ref, mode_ref, table_ref, g_k_ref, g_kq_ref, dmat_ref,
    proj_ref, spread_ref, same_ref, beta_k_hbm, beta_kq_hbm,
    out_ref, wave, part, core_in, mine, y_in, y_sum, za_in, za_mid, zb_in, zb_mid, b_sum, b_in,
    coupled, left, total, beta_kq, beta_k, packed, arrived, terms, values, info, send_sem, recv_sem, load_sem,
):
    me = lax.axis_index("ga")
    n = layout.groups
    c, y, z = me % 2, (me // 2) % 2, me // 4

    def index(zz, yy, cc):
        return (zz * 2 + yy) * 2 + cc

    up, down, far = (z + 1) % RING, (z + RING - 1) % RING, (z + 2) % RING
    other_core, other_y = index(z, y, 1 - c), index(z, 1 - y, c)
    next_z, last_z = index(up, y, c), index(down, y, c)
    load_k = pltpu.make_async_copy(beta_k_hbm, beta_k, load_sem.at[0])
    load_k.start()
    load = pltpu.make_async_copy(beta_kq_hbm, beta_kq, load_sem.at[1])
    load.start()

    barrier = pltpu.get_barrier_semaphore()
    for step in range(1, n):
        pl.semaphore_signal(
            barrier, inc=1, device_id={"ga": (me + step) % n}, device_id_type=pl.DeviceIdType.MESH
        )
    rows_here, slots = psi_ref.shape[1], n * send_ref.shape[1]
    cap = send_ref.shape[1]
    pick = (lax.broadcasted_iota(jnp.int32, (rows_here, slots), 0) == slot_row(send_ref)).astype(BF16)
    for k in range(2):
        width = psi_ref.shape[2]
        packed[:, :, k * width:(k + 1) * width] = dot_t(pick, psi_ref[k]).astype(BF16).reshape(n, cap, width)
    pl.semaphore_wait(barrier, n - 1)

    sends = Sends(send_sem, recv_sem)
    rows = layout.rows
    bands = wave.shape[1] // 2
    half = 2 * bands
    low, high = pl.ds(0, half), pl.ds(half, half)
    left_cols, right_cols = pl.ds(0, bands), pl.ds(bands, bands)
    high_left, high_right = pl.ds(half, bands), pl.ds(half + bands, bands)

    def add(first, *others):
        value = first.astype(F32)
        for other in others:
            value = value + other.astype(F32)
        return value

    psi_copies = [
        sends.start(packed.at[(me + step) % n], arrived.at[me], (me + step) % n) for step in far_first(n)
    ]
    arrived[me] = packed[me]
    sorted_info(layout, displaced_ref, mode_ref, table_ref, values, info)
    load_k.wait()
    for b in range(RING):
        for k, term in enumerate(selected_terms(layout, beta_k, info[b], g_k_ref, b)):
            terms[b, k] = term.astype(BF16)
    load.wait()
    prepare_block(layout, beta_kq, info[0], g_kq_ref, left, 0)
    for copy in psi_copies:
        copy.wait_recv()

    pick = (lax.broadcasted_iota(jnp.int32, (slots, rows_here), 0) == slot_ref[...]).astype(BF16)
    wave[...] = dot_t(pick, arrived[...].reshape(slots, 2 * bands)).astype(BF16)
    order = (far, up, down, z)
    core_copies, y_copies, z_copies = [], [], []

    def settle(i):
        b = order[i]
        for yy in range(2):
            core_copies[i][yy].wait_recv()
            mine[b, yy] = add(part[b, yy, c], core_in[b, yy]).astype(BF16)
        if i == 0:
            z_copies.append(sends.start(mine.at[b, :, :, high_left], zb_in.at[0], next_z))
            z_copies.append(sends.start(mine.at[b, :, :, high_right], zb_in.at[1], last_z))
        if i == 1:
            z_copies.append(sends.start(mine.at[b, :, :, high_right], zb_in.at[2], next_z))
        if i == 2:
            z_copies.append(sends.start(mine.at[b, :, :, high_left], zb_in.at[3], last_z))
        y_copies.append(sends.start(mine.at[b, 1 - y, :, low], y_in.at[b], other_y))

    for i, b in enumerate(order):

        def store(k, value, b=b):
            for yy in range(2):
                for cc in range(2):
                    at = (yy * 2 + cc) * rows
                    part[b, yy, cc, :, k * bands:(k + 1) * bands] = value[at:at + rows]

        project_block([terms[b, k] for k in range(4)], wave[...], store)
        core_copies.append([
            sends.start(part.at[b, yy, 1 - c], core_in.at[b, yy], other_core) for yy in range(2)
        ])
        if i > 0:
            settle(i - 1)
    settle(RING - 1)
    zb_up, zb_down, zb_up_own, zb_down_own = z_copies

    def y_settle(i):
        b = order[i]
        y_copies[i].wait_recv()
        y_sum[b] = add(mine[b, y, :, :half], y_in[b]).astype(BF16)

    shard_atom = info[z, pl.ds(pl.multiple_of((y * 2 + c) * rows, 8), rows), 7:8]
    coupling = coupling_matrix(layout, dmat_ref, shard_atom, proj_ref[...], spread_ref, same_ref)
    zb_up.wait_recv()
    zb_mid[0] = add(mine[up, :, :, half:half + bands], zb_in[0]).astype(BF16)
    zb_up_sum = sends.start(zb_mid.at[0], zb_in.at[4], next_z)
    zb_down.wait_recv()
    zb_mid[1] = add(mine[down, :, :, half + bands:], zb_in[1]).astype(BF16)
    zb_down_sum = sends.start(zb_mid.at[1], zb_in.at[5], last_z)

    y_settle(0)
    za_up = sends.start(y_sum.at[far, :, left_cols], za_in.at[0], next_z)
    za_down = sends.start(y_sum.at[far, :, right_cols], za_in.at[1], last_z)
    prepare_block(layout, beta_kq, info[1], g_kq_ref, left, 1)
    y_settle(1)
    za_up_own = sends.start(y_sum.at[up, :, right_cols], za_in.at[2], next_z)
    y_settle(2)
    za_down_own = sends.start(y_sum.at[down, :, left_cols], za_in.at[3], last_z)
    prepare_block(layout, beta_kq, info[2], g_kq_ref, left, 2)

    for copy in (zb_up_own, zb_down_own, zb_up_sum, zb_down_sum):
        copy.wait_recv()
    b_sum[:, :, :bands] = add(mine[z, :, :, half:half + bands], zb_in[4], zb_in[3]).astype(BF16)
    b_sum[:, :, bands:] = add(mine[z, :, :, half + bands:], zb_in[5], zb_in[2]).astype(BF16)
    b_y = sends.start(b_sum.at[1 - y], b_in, other_y)

    za_up.wait_recv()
    za_mid[0] = add(y_sum[up, :, :bands], za_in[0]).astype(BF16)
    za_up_sum = sends.start(za_mid.at[0], za_in.at[4], next_z)
    za_down.wait_recv()
    za_mid[1] = add(y_sum[down, :, bands:], za_in[1]).astype(BF16)
    za_down_sum = sends.start(za_mid.at[1], za_in.at[5], last_z)
    y_settle(3)

    prepare_block(layout, beta_kq, info[3], g_kq_ref, left, 3)

    def couple(value):
        return exact_dot(coupling, value).astype(BF16)

    b_y.wait_recv()
    coupled[z, y, c, :, half:] = couple(add(b_sum[y], b_in[...]))
    own = coupled.at[z, y, c, :, high]
    gb_y = sends.start(own, own, other_y)
    for copy in (za_up_own, za_down_own, za_up_sum, za_down_sum):
        copy.wait_recv()
    coupled[z, y, c, :, :bands] = couple(add(y_sum[z, :, :bands], za_in[4], za_in[3]))
    coupled[z, y, c, :, bands:half] = couple(add(y_sum[z, :, bands:], za_in[5], za_in[2]))

    own = coupled.at[z, y, c, :, low]
    ga_up = sends.start(own, own, next_z)
    ga_down = sends.start(own, own, last_z)
    ga_y = [sends.start(own, own, other_y)]
    gc = [sends.start(coupled.at[z, y, c], coupled.at[z, y, c], other_core)]
    gb_y.wait_recv()
    pair = coupled.at[z, :, c, :, high]
    gb_up = sends.start(pair, pair, next_z)
    gb_down = sends.start(pair, pair, last_z)

    def forward(ref, device):
        return sends.start(ref, ref, device)

    ga_up.wait_recv()
    from_down_a = coupled.at[down, y, c, :, low]
    ga_up2 = forward(coupled.at[down, y, c, :, left_cols], next_z)
    ga_y.append(forward(from_down_a, other_y))
    ga_down.wait_recv()
    from_up_a = coupled.at[up, y, c, :, low]
    ga_down2 = forward(coupled.at[up, y, c, :, right_cols], last_z)
    ga_y.append(forward(from_up_a, other_y))
    ga_y[0].wait_recv()
    gc.append(forward(coupled.at[z, 1 - y, c], other_core))

    gb_up.wait_recv()
    gb_up2 = forward(coupled.at[down, :, c, :, high_left], next_z)
    gc_down = forward(coupled.at[down, :, c, :, high], other_core)
    gb_down.wait_recv()
    gb_down2 = forward(coupled.at[up, :, c, :, high_right], last_z)
    gc_up = forward(coupled.at[up, :, c, :, high], other_core)

    def back(b, first):
        parts = back_block(left, b, coupled[b].reshape(layout.block, 2 * half))
        for k in range(2):
            total[k] = parts[k] if first else total[k] + parts[k]

    for copy in gc:
        copy.wait_recv()
    back(z, True)

    ga_up2.wait_recv()
    ga_down2.wait_recv()
    ga_y.append(forward(coupled.at[far, y, c, :, low], other_y))
    ga_y[1].wait_recv()
    gc_down_a = forward(coupled.at[down, :, c, :, low], other_core)
    ga_y[2].wait_recv()
    gc_up_a = forward(coupled.at[up, :, c, :, low], other_core)
    gc_down.wait_recv()
    gc_down_a.wait_recv()
    back(down, False)
    gb_up2.wait_recv()
    gb_down2.wait_recv()
    gc_far = forward(coupled.at[far, :, c, :, high], other_core)
    ga_y[3].wait_recv()
    gc_far_a = forward(coupled.at[far, :, c, :, low], other_core)
    gc_up.wait_recv()
    gc_up_a.wait_recv()
    back(up, False)
    gc_far.wait_recv()
    gc_far_a.wait_recv()
    parts = back_block(left, far, coupled[far].reshape(layout.block, 2 * half))
    for k in range(2):
        out_ref[k] = (total[k] + parts[k]).astype(BF16)
    sends.finish()


COPIES = 80


def far_first(n):
    return sorted(range(1, n), key=lambda step: -min(step, n - step))


def tables(layout):
    row = np.arange(layout.rows)
    valid = row < layout.used
    slot = np.where(valid, row // layout.per_atom, 0)
    proj = np.where(valid, row % layout.per_atom, -1)
    table = np.zeros((8, layout.blocks, layout.padded), np.float32)
    table[0] = -1.0
    for b in range(layout.blocks):
        for k in range(layout.gang):
            at = slice(k * layout.rows, (k + 1) * layout.rows)
            table[0, b, at] = np.where(valid, (b * layout.gang + k) * layout.per_shard + slot, -1)
            table[1, b, at] = np.where(valid, proj, 0)
    spread = (np.arange(layout.per_atom)[:, None] == proj[None]).astype(np.float32)
    same = (slot[:, None] == slot[None]) & valid[:, None] & valid[None]
    return (
        table.reshape(8, -1),
        proj[:, None].astype(np.int32),
        spread,
        same.astype(np.float32),
    )


def fused(layout, psi_k, send_index, recv_index, beta_k, beta_kq, displaced, mode, g_k, g_kq, dmat):
    rows, bands = psi_k.shape[1:]
    width = 2 * bands
    cap = send_index.shape[2]
    table, proj, spread, same = (jnp.asarray(value) for value in tables(layout))
    r = layout.rows
    vmem = pl.BlockSpec(memory_space=pltpu.VMEM)

    def buffer(*shape, dtype=BF16):
        return pltpu.VMEM(shape, dtype)

    return pl.pallas_call(
        functools.partial(fused_kernel, layout),
        in_specs=[vmem] * 12 + [pl.BlockSpec(memory_space=pl.ANY)] * 2,
        out_specs=vmem,
        out_shape=jax.ShapeDtypeStruct((2, rows, bands), BF16),
        scratch_shapes=[
            buffer(rows, width),
            buffer(RING, 2, 2, r, 2 * width),
            buffer(RING, 2, r, 2 * width),
            buffer(RING, 2, r, 2 * width),
            buffer(RING, r, width),
            buffer(RING, r, width),
            buffer(6, r, bands),
            buffer(2, r, bands),
            buffer(6, 2, r, bands),
            buffer(2, 2, r, bands),
            buffer(2, r, width),
            buffer(r, width),
            buffer(RING, 2, 2, r, 2 * width),
            buffer(RING, 4, rows, layout.block),
            buffer(2, rows, bands, dtype=F32),
            pltpu.VMEM(beta_kq.shape, BF16),
            pltpu.VMEM(beta_k.shape, BF16),
            buffer(layout.groups, cap, width),
            buffer(layout.groups, cap, width),
            buffer(RING, 4, layout.block, rows),
            buffer(8, displaced.shape[0], dtype=F32),
            buffer(RING, layout.block, 8, dtype=F32),
            pltpu.SemaphoreType.DMA((COPIES,)),
            pltpu.SemaphoreType.DMA((COPIES,)),
            pltpu.SemaphoreType.DMA((2,)),
        ],
        compiler_params=params(collective_id=0, has_side_effects=True),
    )(
        psi_k, send_index[0], recv_index.reshape(1, -1), displaced.reshape(1, -1), mode, table, g_k, g_kq,
        jnp.transpose(dmat, (1, 2, 0)), proj, spread, same, beta_k, beta_kq,
    )


def pad_rows(layout, values, fill):
    k = values.shape[0]
    parts = values.reshape(k, layout.groups, layout.used)
    parts = jnp.pad(parts, ((0, 0), (0, 0), (0, layout.rows - layout.used)), constant_values=fill)
    parts = parts.reshape(k, layout.blocks, layout.block)
    parts = jnp.pad(parts, ((0, 0), (0, 0), (0, layout.padded - layout.block)), constant_values=fill)
    return parts.reshape(k, layout.blocks * layout.padded)


def block_coupling(layout, dmat, atoms):
    mine = lax.dynamic_slice_in_dim(atoms, lax.axis_index("ga") * layout.per_shard, layout.per_shard)
    blocks = jnp.take(dmat, mine, axis=0)
    eye = jnp.eye(layout.per_shard, dtype=F32)
    full = (blocks[:, :, None, :] * eye[:, None, :, None]).reshape(layout.used, layout.used)
    extra = layout.rows - layout.used
    return jnp.pad(full, ((0, extra), (0, extra)))


def on_device(psi_k, beta_k, beta_kq, g_k, g_kq, send_index, recv_index, dmat, displaced, mode):
    groups = lax.axis_size("ga")
    total = beta_k.shape[2]
    rows = beta_k.shape[1]
    per_atom = dmat.shape[1]
    layout = Layout(groups, displaced.shape[0], per_atom, total)

    beta_k, beta_kq = jnp.transpose(beta_k, (0, 2, 1)), jnp.transpose(beta_kq, (0, 2, 1))
    if groups == RING * CORE_Y:
        return fused(layout, psi_k, send_index, recv_index, beta_k, beta_kq, displaced, mode, g_k, g_kq, dmat)

    packed = pack_rows(send_index.reshape(1, -1), psi_k)
    arrived = lax.all_to_all(packed, "ga", split_axis=0, concat_axis=0, tiled=True)

    rank = jnp.sum((displaced[None, :] < displaced[:, None]).astype(jnp.int32), axis=1)
    place = rank[None, :] == jnp.arange(displaced.shape[0], dtype=jnp.int32)[:, None]
    atoms = jnp.sum(jnp.where(place, displaced[None, :], 0), axis=1)
    moves = jnp.sum(jnp.where(place[None], mode[:, None, :], 0.0), axis=2)
    steps = jnp.tile(jnp.arange(per_atom, dtype=F32), displaced.shape[0])
    source = jnp.repeat(atoms.astype(F32) * per_atom, per_atom) + steps
    source = pad_rows(layout, source[None], -1.0)
    weights = pad_rows(layout, jnp.repeat(moves, per_atom, axis=1), 0.0)
    filler = jnp.zeros((8 - 1 - weights.shape[0], source.shape[1]), F32)
    info = jnp.concatenate([source, weights, filler], axis=0)
    coupling = block_coupling(layout, dmat, atoms)
    return separate_steps(
        layout, arrived, recv_index.reshape(1, -1), beta_k, beta_kq, info, g_k, g_kq, coupling
    )


def solution(mesh):
    in_specs = (
        P(None, "ga", None),
        P(None, "ga", None),
        P(None, "ga", None),
        P(None, "ga"),
        P(None, "ga"),
        P("ga", None, None),
        P("ga"),
        P(),
        P("pert"),
        P(None, "pert"),
    )
    out_specs = P("pert", "ga", None)
    return jax.shard_map(
        on_device, mesh=mesh, in_specs=in_specs, out_specs=out_specs, check_vma=False
    )
```

```python
import functools

import jax
import jax.numpy as jnp
import numpy as np
from jax import lax
from jax.experimental import pallas as pl
from jax.experimental.pallas import tpu as pltpu
from jax.sharding import PartitionSpec as P

LANES = 128
RING = 4
CORE_Y = 4
BF16 = jnp.bfloat16
F32 = jnp.float32
VMEM_LIMIT = 56 * 1024 * 1024


def round_up(value, step):
    return -(-value // step) * step


def dot(a, b):
    return jnp.dot(a, b, preferred_element_type=F32)


def dot_t(a, b):
    return lax.dot_general(a, b, (((0,), (0,)), ((), ())), preferred_element_type=F32)


def pack_kernel(slot_ref, psi_ref, out_ref):
    rows = psi_ref.shape[1]
    bands = psi_ref.shape[2]
    slots = slot_ref.shape[1]
    pick = (lax.broadcasted_iota(jnp.int32, (rows, slots), 0) == slot_ref[...]).astype(BF16)
    for part in range(2):
        out_ref[:, part * bands:(part + 1) * bands] = dot_t(pick, psi_ref[part]).astype(BF16)


def pack_rows(slots, psi_k):
    return pl.pallas_call(
        pack_kernel,
        out_shape=jax.ShapeDtypeStruct((slots.shape[1], 2 * psi_k.shape[2]), BF16),
        compiler_params=pltpu.CompilerParams(vmem_limit_bytes=VMEM_LIMIT),
    )(slots, psi_k)


class Layout:
    def __init__(self, groups, atoms, per_atom, total):
        self.groups = groups
        self.blocks = groups // CORE_Y
        self.gang = CORE_Y
        if self.blocks != RING:
            self.blocks = RING
            self.gang = groups // RING
        self.per_shard = atoms // groups
        self.per_atom = per_atom
        self.used = self.per_shard * per_atom
        self.rows = round_up(self.used, 16)
        self.block = self.gang * self.rows
        self.padded = round_up(self.block, LANES)
        self.total = total
        slack = total - atoms * per_atom
        self.window = min(total, round_up(self.gang * self.used + slack + 16, LANES))
        self.starts = [
            min(b * self.gang * self.used // 16 * 16, total - self.window) for b in range(self.blocks)
        ]


def columns_of(layout, info_ref, b):
    wide = info_ref[:, b * layout.padded:(b + 1) * layout.padded]
    return jnp.transpose(wide)[: layout.block]


def select(layout, beta_ref, info, b):
    start = layout.starts[b]
    ids = lax.broadcasted_iota(jnp.int32, (layout.block, layout.window), 1) + start
    pick = (ids == info[:, 0:1].astype(jnp.int32)).astype(BF16)
    rows = pl.ds(start, layout.window)
    return dot(pick, beta_ref[0, rows, :]), dot(pick, beta_ref[1, rows, :])


def row_scale(g_ref, info):
    total = info[:, 1:2] * g_ref[0:1, :]
    for x in range(1, g_ref.shape[0]):
        total = total + info[:, x + 1:x + 2] * g_ref[x:x + 1, :]
    return total


def regroup(arrived_ref, slot_ref, wave):
    slots, rows = arrived_ref.shape[0], wave.shape[0]
    pick = (lax.broadcasted_iota(jnp.int32, (slots, rows), 0) == slot_ref[...]).astype(BF16)
    wave[...] = dot_t(pick, arrived_ref[...]).astype(BF16)


def selected_terms(layout, beta_ref, info, g_ref, b):
    real, imag = select(layout, beta_ref, info, b)
    scale = row_scale(g_ref, info)
    return real, imag, scale * imag, scale * real


def project_block(terms, stacked, store):
    bands = stacked.shape[1] // 2
    x = dot(terms[0], stacked)
    y = dot(terms[1], stacked)
    store(0, (x[:, :bands] + y[:, bands:]).astype(BF16))
    store(1, (x[:, bands:] - y[:, :bands]).astype(BF16))
    x = dot(terms[2], stacked)
    y = dot(terms[3], stacked)
    store(2, (x[:, :bands] - y[:, bands:]).astype(BF16))
    store(3, (x[:, bands:] + y[:, :bands]).astype(BF16))


def prepare_block(layout, beta_ref, info, g_ref, left_ref, b):
    real, imag, slope_real, slope_imag = selected_terms(layout, beta_ref, info, g_ref, b)
    for k, term in enumerate((slope_real, -slope_imag, real, imag)):
        left_ref[b, k] = term.astype(BF16).T


def back_block(left_ref, b, coupled):
    width = coupled.shape[1] // 2
    bands = width // 2
    first, second = coupled[:, :width], coupled[:, width:]
    x = dot(left_ref[b, 0], first) + dot(left_ref[b, 2], second)
    y = dot(left_ref[b, 1], first) + dot(left_ref[b, 3], second)
    return x[:, :bands] - y[:, bands:], x[:, bands:] + y[:, :bands]


def project_kernel(layout, arrived_ref, slot_ref, beta_ref, info_ref, g_ref, out_ref, wave):
    regroup(arrived_ref, slot_ref, wave)
    bands = wave.shape[1] // 2
    for b in range(layout.blocks):

        def store(k, value, b=b):
            out_ref[b * layout.block:(b + 1) * layout.block, k * bands:(k + 1) * bands] = value

        info = columns_of(layout, info_ref, b)
        terms = [term.astype(BF16) for term in selected_terms(layout, beta_ref, info, g_ref, b)]
        project_block(terms, wave[...], store)


def finish_kernel(layout, beta_ref, info_ref, g_ref, coupled_ref, out_ref, left, total):
    for b in range(layout.blocks):
        prepare_block(layout, beta_ref, columns_of(layout, info_ref, b), g_ref, left, b)
        parts = back_block(left, b, coupled_ref[b * layout.block:(b + 1) * layout.block, :])
        for k in range(2):
            total[k] = parts[k] if b == 0 else total[k] + parts[k]
    out_ref[...] = total[...].astype(BF16)


def params(**extra):
    return pltpu.CompilerParams(vmem_limit_bytes=VMEM_LIMIT, **extra)


def separate_steps(layout, arrived, slots, beta_k, beta_kq, info, g_k, g_kq, coupling):
    rows, width = slots.shape[1], arrived.shape[1]
    terms = pl.pallas_call(
        functools.partial(project_kernel, layout),
        out_shape=jax.ShapeDtypeStruct((layout.groups * layout.rows, 2 * width), BF16),
        scratch_shapes=[pltpu.VMEM((rows, width), BF16)],
        compiler_params=params(),
    )(arrived, slots, beta_k, info, g_k)
    shard = lax.psum_scatter(terms.astype(F32), "ga", scatter_dimension=0, tiled=True)
    mixed = jnp.dot(
        coupling, shard, precision=lax.Precision.HIGHEST, preferred_element_type=F32
    ).astype(BF16)
    coupled = lax.all_gather(mixed, "ga", axis=0, tiled=True)
    return pl.pallas_call(
        functools.partial(finish_kernel, layout),
        out_shape=jax.ShapeDtypeStruct((2, rows, width // 2), BF16),
        scratch_shapes=[
            pltpu.VMEM((layout.blocks, 4, rows, layout.block), BF16),
            pltpu.VMEM((2, rows, width // 2), F32),
        ],
        compiler_params=params(),
    )(beta_kq, info, g_kq, coupled)


class Sends:
    def __init__(self, send_sem, recv_sem):
        self.send_sem, self.recv_sem = send_sem, recv_sem
        self.started = []

    def start(self, source, target, device):
        k = len(self.started)
        copy = pltpu.make_async_remote_copy(
            src_ref=source,
            dst_ref=target,
            send_sem=self.send_sem.at[k],
            recv_sem=self.recv_sem.at[k],
            device_id={"ga": device},
            device_id_type=pl.DeviceIdType.MESH,
        )
        copy.start()
        self.started.append(copy)
        return copy

    def finish(self):
        for copy in self.started:
            copy.wait_send()


def exact_dot(a, b):
    return jnp.dot(a, b, precision=lax.Precision.HIGHEST, preferred_element_type=F32)


def slot_row(send_ref):
    receivers, cap = send_ref.shape
    column = lax.broadcasted_iota(jnp.int32, (cap, receivers * cap), 1)
    inner = lax.broadcasted_iota(jnp.int32, (cap, receivers * cap), 0)
    wide = exact_dot(send_ref[...].astype(F32), (column % cap == inner).astype(F32))
    column = lax.broadcasted_iota(jnp.int32, wide.shape, 1)
    outer = lax.broadcasted_iota(jnp.int32, wide.shape, 0)
    return jnp.sum(jnp.where(column // cap == outer, wide, 0.0), axis=0, keepdims=True).astype(jnp.int32)


def sorted_info(layout, displaced_ref, mode_ref, table_ref, values, info):
    parts = mode_ref.shape[0]
    values[...] = jnp.zeros_like(values)
    values[0:1, :] = displaced_ref[...].astype(F32)
    values[1:1 + parts, :] = mode_ref[...]
    by_atom = jnp.transpose(values[...])
    smaller = (by_atom[:, 0:1] < values[0:1, :]).astype(F32)
    rank = jnp.sum(smaller, axis=0, keepdims=True)
    lane = lax.broadcasted_iota(jnp.int32, (layout.block, values.shape[0]), 1)
    for b in range(layout.blocks):
        place = columns_of(layout, table_ref, b)
        found = exact_dot((place[:, 0:1] == rank).astype(F32), by_atom)
        source = jnp.where(place[:, 0:1] < 0, -1.0, found * layout.per_atom + place[:, 1:2])
        info[b] = jnp.where(lane == 0, source, jnp.where(lane == 7, found[:, 0:1], found))


def coupling_matrix(layout, dmat_ref, atom, proj, spread_ref, same_ref):
    lanes = lax.broadcasted_iota(jnp.int32, (layout.rows, dmat_ref.shape[2]), 1)
    pick = (lanes == atom.astype(jnp.int32)).astype(F32)
    rows = jnp.zeros((layout.rows, layout.per_atom), F32)
    for i in range(layout.per_atom):
        found = lax.dot_general(
            pick, dmat_ref[i], (((1,), (1,)), ((), ())),
            precision=lax.Precision.HIGHEST, preferred_element_type=F32,
        )
        rows = rows + jnp.where(proj == i, found, 0.0)
    return exact_dot(rows, spread_ref[...]) * same_ref[...]


def fused_kernel(
    layout, psi_ref, send_ref, slot_ref, displaced_ref, mode_ref, table_ref, g_k_ref, g_kq_ref, dmat_ref,
    proj_ref, spread_ref, same_ref, beta_k_hbm, beta_kq_hbm,
    out_ref, wave, part, core_in, mine, y_in, y_sum, za_in, za_mid, zb_in, zb_mid, b_sum, b_in,
    coupled, left, total, beta_kq, beta_k, packed, arrived, terms, values, info, send_sem, recv_sem, load_sem,
):
    me = lax.axis_index("ga")
    n = layout.groups
    c, y, z = me % 2, (me // 2) % 2, me // 4

    def index(zz, yy, cc):
        return (zz * 2 + yy) * 2 + cc

    up, down, far = (z + 1) % RING, (z + RING - 1) % RING, (z + 2) % RING
    other_core, other_y = index(z, y, 1 - c), index(z, 1 - y, c)
    next_z, last_z = index(up, y, c), index(down, y, c)
    load_k = pltpu.make_async_copy(beta_k_hbm, beta_k, load_sem.at[0])
    load_k.start()
    load = pltpu.make_async_copy(beta_kq_hbm, beta_kq, load_sem.at[1])
    load.start()

    barrier = pltpu.get_barrier_semaphore()
    for step in range(1, n):
        pl.semaphore_signal(
            barrier, inc=1, device_id={"ga": (me + step) % n}, device_id_type=pl.DeviceIdType.MESH
        )
    rows_here, slots = psi_ref.shape[1], n * send_ref.shape[1]
    cap = send_ref.shape[1]
    pick = (lax.broadcasted_iota(jnp.int32, (rows_here, slots), 0) == slot_row(send_ref)).astype(BF16)
    for k in range(2):
        width = psi_ref.shape[2]
        packed[:, :, k * width:(k + 1) * width] = dot_t(pick, psi_ref[k]).astype(BF16).reshape(n, cap, width)
    pl.semaphore_wait(barrier, n - 1)

    sends = Sends(send_sem, recv_sem)
    rows = layout.rows
    bands = wave.shape[1] // 2
    half = 2 * bands
    low, high = pl.ds(0, half), pl.ds(half, half)
    left_cols, right_cols = pl.ds(0, bands), pl.ds(bands, bands)
    high_left, high_right = pl.ds(half, bands), pl.ds(half + bands, bands)

    def add(first, *others):
        value = first.astype(F32)
        for other in others:
            value = value + other.astype(F32)
        return value

    psi_copies = [
        sends.start(packed.at[(me + step) % n], arrived.at[me], (me + step) % n) for step in far_first(n)
    ]
    arrived[me] = packed[me]
    sorted_info(layout, displaced_ref, mode_ref, table_ref, values, info)
    load_k.wait()
    for b in range(RING):
        for k, term in enumerate(selected_terms(layout, beta_k, info[b], g_k_ref, b)):
            terms[b, k] = term.astype(BF16)
    load.wait()
    prepare_block(layout, beta_kq, info[0], g_kq_ref, left, 0)
    prepare_block(layout, beta_kq, info[1], g_kq_ref, left, 1)
    shard_atom = info[z, pl.ds(pl.multiple_of((y * 2 + c) * rows, 8), rows), 7:8]
    coupling = coupling_matrix(layout, dmat_ref, shard_atom, proj_ref[...], spread_ref, same_ref)
    for copy in psi_copies:
        copy.wait_recv()

    pick = (lax.broadcasted_iota(jnp.int32, (slots, rows_here), 0) == slot_ref[...]).astype(BF16)
    wave[...] = dot_t(pick, arrived[...].reshape(slots, 2 * bands)).astype(BF16)
    order = (far, up, down, z)
    core_copies, y_copies, z_copies = [], [], []

    def settle(i):
        b = order[i]
        for yy in range(2):
            core_copies[i][yy].wait_recv()
            mine[b, yy] = add(part[b, yy, c], core_in[b, yy]).astype(BF16)
        if i == 0:
            z_copies.append(sends.start(mine.at[b, :, :, high_left], zb_in.at[0], next_z))
            z_copies.append(sends.start(mine.at[b, :, :, high_right], zb_in.at[1], last_z))
        if i == 1:
            z_copies.append(sends.start(mine.at[b, :, :, high_right], zb_in.at[2], next_z))
        if i == 2:
            z_copies.append(sends.start(mine.at[b, :, :, high_left], zb_in.at[3], last_z))
        y_copies.append(sends.start(mine.at[b, 1 - y, :, low], y_in.at[b], other_y))

    for i, b in enumerate(order):

        def store(k, value, b=b):
            for yy in range(2):
                for cc in range(2):
                    at = (yy * 2 + cc) * rows
                    part[b, yy, cc, :, k * bands:(k + 1) * bands] = value[at:at + rows]

        project_block([terms[b, k] for k in range(4)], wave[...], store)
        core_copies.append([
            sends.start(part.at[b, yy, 1 - c], core_in.at[b, yy], other_core) for yy in range(2)
        ])
        if i > 0:
            settle(i - 1)
    settle(RING - 1)
    zb_up, zb_down, zb_up_own, zb_down_own = z_copies

    def y_settle(i):
        b = order[i]
        y_copies[i].wait_recv()
        y_sum[b] = add(mine[b, y, :, :half], y_in[b]).astype(BF16)

    zb_up.wait_recv()
    zb_mid[0] = add(mine[up, :, :, half:half + bands], zb_in[0]).astype(BF16)
    zb_up_sum = sends.start(zb_mid.at[0], zb_in.at[4], next_z)
    zb_down.wait_recv()
    zb_mid[1] = add(mine[down, :, :, half + bands:], zb_in[1]).astype(BF16)
    zb_down_sum = sends.start(zb_mid.at[1], zb_in.at[5], last_z)

    y_settle(0)
    za_up = sends.start(y_sum.at[far, :, left_cols], za_in.at[0], next_z)
    za_down = sends.start(y_sum.at[far, :, right_cols], za_in.at[1], last_z)
    y_settle(1)
    za_up_own = sends.start(y_sum.at[up, :, right_cols], za_in.at[2], next_z)
    y_settle(2)
    za_down_own = sends.start(y_sum.at[down, :, left_cols], za_in.at[3], last_z)
    prepare_block(layout, beta_kq, info[2], g_kq_ref, left, 2)

    for copy in (zb_up_own, zb_down_own, zb_up_sum, zb_down_sum):
        copy.wait_recv()
    b_sum[:, :, :bands] = add(mine[z, :, :, half:half + bands], zb_in[4], zb_in[3]).astype(BF16)
    b_sum[:, :, bands:] = add(mine[z, :, :, half + bands:], zb_in[5], zb_in[2]).astype(BF16)
    b_y = sends.start(b_sum.at[1 - y], b_in, other_y)

    za_up.wait_recv()
    za_mid[0] = add(y_sum[up, :, :bands], za_in[0]).astype(BF16)
    za_up_sum = sends.start(za_mid.at[0], za_in.at[4], next_z)
    za_down.wait_recv()
    za_mid[1] = add(y_sum[down, :, bands:], za_in[1]).astype(BF16)
    za_down_sum = sends.start(za_mid.at[1], za_in.at[5], last_z)
    y_settle(3)

    prepare_block(layout, beta_kq, info[3], g_kq_ref, left, 3)

    def couple(value):
        return exact_dot(coupling, value).astype(BF16)

    b_y.wait_recv()
    coupled[z, y, c, :, half:] = couple(add(b_sum[y], b_in[...]))
    own = coupled.at[z, y, c, :, high]
    gb_y = sends.start(own, own, other_y)
    for copy in (za_up_own, za_down_own, za_up_sum, za_down_sum):
        copy.wait_recv()
    coupled[z, y, c, :, :bands] = couple(add(y_sum[z, :, :bands], za_in[4], za_in[3]))
    coupled[z, y, c, :, bands:half] = couple(add(y_sum[z, :, bands:], za_in[5], za_in[2]))

    own = coupled.at[z, y, c, :, low]
    ga_up = sends.start(own, own, next_z)
    ga_down = sends.start(own, own, last_z)
    ga_y = [sends.start(own, own, other_y)]
    gc = [sends.start(coupled.at[z, y, c], coupled.at[z, y, c], other_core)]
    gb_y.wait_recv()
    pair = coupled.at[z, :, c, :, high]
    gb_up = sends.start(pair, pair, next_z)
    gb_down = sends.start(pair, pair, last_z)

    def forward(ref, device):
        return sends.start(ref, ref, device)

    ga_up.wait_recv()
    from_down_a = coupled.at[down, y, c, :, low]
    ga_up2 = forward(coupled.at[down, y, c, :, left_cols], next_z)
    ga_y.append(forward(from_down_a, other_y))
    ga_down.wait_recv()
    from_up_a = coupled.at[up, y, c, :, low]
    ga_down2 = forward(coupled.at[up, y, c, :, right_cols], last_z)
    ga_y.append(forward(from_up_a, other_y))
    ga_y[0].wait_recv()
    gc.append(forward(coupled.at[z, 1 - y, c], other_core))

    gb_up.wait_recv()
    gb_up2 = forward(coupled.at[down, :, c, :, high_left], next_z)
    gc_down = forward(coupled.at[down, :, c, :, high], other_core)
    gb_down.wait_recv()
    gb_down2 = forward(coupled.at[up, :, c, :, high_right], last_z)
    gc_up = forward(coupled.at[up, :, c, :, high], other_core)

    def back(b, first):
        parts = back_block(left, b, coupled[b].reshape(layout.block, 2 * half))
        for k in range(2):
            total[k] = parts[k] if first else total[k] + parts[k]

    for copy in gc:
        copy.wait_recv()
    back(z, True)

    ga_up2.wait_recv()
    ga_down2.wait_recv()
    ga_y.append(forward(coupled.at[far, y, c, :, low], other_y))
    ga_y[1].wait_recv()
    gc_down_a = forward(coupled.at[down, :, c, :, low], other_core)
    ga_y[2].wait_recv()
    gc_up_a = forward(coupled.at[up, :, c, :, low], other_core)
    gc_down.wait_recv()
    gc_down_a.wait_recv()
    back(down, False)
    gb_up2.wait_recv()
    gb_down2.wait_recv()
    gc_far = forward(coupled.at[far, :, c, :, high], other_core)
    ga_y[3].wait_recv()
    gc_far_a = forward(coupled.at[far, :, c, :, low], other_core)
    gc_up.wait_recv()
    gc_up_a.wait_recv()
    back(up, False)
    gc_far.wait_recv()
    gc_far_a.wait_recv()
    parts = back_block(left, far, coupled[far].reshape(layout.block, 2 * half))
    for k in range(2):
        out_ref[k] = (total[k] + parts[k]).astype(BF16)
    sends.finish()


COPIES = 80


def far_first(n):
    return sorted(range(1, n), key=lambda step: -min(step, n - step))


def tables(layout):
    row = np.arange(layout.rows)
    valid = row < layout.used
    slot = np.where(valid, row // layout.per_atom, 0)
    proj = np.where(valid, row % layout.per_atom, -1)
    table = np.zeros((8, layout.blocks, layout.padded), np.float32)
    table[0] = -1.0
    for b in range(layout.blocks):
        for k in range(layout.gang):
            at = slice(k * layout.rows, (k + 1) * layout.rows)
            table[0, b, at] = np.where(valid, (b * layout.gang + k) * layout.per_shard + slot, -1)
            table[1, b, at] = np.where(valid, proj, 0)
    spread = (np.arange(layout.per_atom)[:, None] == proj[None]).astype(np.float32)
    same = (slot[:, None] == slot[None]) & valid[:, None] & valid[None]
    return (
        table.reshape(8, -1),
        proj[:, None].astype(np.int32),
        spread,
        same.astype(np.float32),
    )


def fused(layout, psi_k, send_index, recv_index, beta_k, beta_kq, displaced, mode, g_k, g_kq, dmat):
    rows, bands = psi_k.shape[1:]
    width = 2 * bands
    cap = send_index.shape[2]
    table, proj, spread, same = (jnp.asarray(value) for value in tables(layout))
    r = layout.rows
    vmem = pl.BlockSpec(memory_space=pltpu.VMEM)

    def buffer(*shape, dtype=BF16):
        return pltpu.VMEM(shape, dtype)

    return pl.pallas_call(
        functools.partial(fused_kernel, layout),
        in_specs=[vmem] * 12 + [pl.BlockSpec(memory_space=pl.ANY)] * 2,
        out_specs=vmem,
        out_shape=jax.ShapeDtypeStruct((2, rows, bands), BF16),
        scratch_shapes=[
            buffer(rows, width),
            buffer(RING, 2, 2, r, 2 * width),
            buffer(RING, 2, r, 2 * width),
            buffer(RING, 2, r, 2 * width),
            buffer(RING, r, width),
            buffer(RING, r, width),
            buffer(6, r, bands),
            buffer(2, r, bands),
            buffer(6, 2, r, bands),
            buffer(2, 2, r, bands),
            buffer(2, r, width),
            buffer(r, width),
            buffer(RING, 2, 2, r, 2 * width),
            buffer(RING, 4, rows, layout.block),
            buffer(2, rows, bands, dtype=F32),
            pltpu.VMEM(beta_kq.shape, BF16),
            pltpu.VMEM(beta_k.shape, BF16),
            buffer(layout.groups, cap, width),
            buffer(layout.groups, cap, width),
            buffer(RING, 4, layout.block, rows),
            buffer(8, displaced.shape[0], dtype=F32),
            buffer(RING, layout.block, 8, dtype=F32),
            pltpu.SemaphoreType.DMA((COPIES,)),
            pltpu.SemaphoreType.DMA((COPIES,)),
            pltpu.SemaphoreType.DMA((2,)),
        ],
        compiler_params=params(collective_id=0, has_side_effects=True),
    )(
        psi_k, send_index[0], recv_index.reshape(1, -1), displaced.reshape(1, -1), mode, table, g_k, g_kq,
        jnp.transpose(dmat, (1, 2, 0)), proj, spread, same, beta_k, beta_kq,
    )


def pad_rows(layout, values, fill):
    k = values.shape[0]
    parts = values.reshape(k, layout.groups, layout.used)
    parts = jnp.pad(parts, ((0, 0), (0, 0), (0, layout.rows - layout.used)), constant_values=fill)
    parts = parts.reshape(k, layout.blocks, layout.block)
    parts = jnp.pad(parts, ((0, 0), (0, 0), (0, layout.padded - layout.block)), constant_values=fill)
    return parts.reshape(k, layout.blocks * layout.padded)


def block_coupling(layout, dmat, atoms):
    mine = lax.dynamic_slice_in_dim(atoms, lax.axis_index("ga") * layout.per_shard, layout.per_shard)
    blocks = jnp.take(dmat, mine, axis=0)
    eye = jnp.eye(layout.per_shard, dtype=F32)
    full = (blocks[:, :, None, :] * eye[:, None, :, None]).reshape(layout.used, layout.used)
    extra = layout.rows - layout.used
    return jnp.pad(full, ((0, extra), (0, extra)))


def on_device(psi_k, beta_k, beta_kq, g_k, g_kq, send_index, recv_index, dmat, displaced, mode):
    groups = lax.axis_size("ga")
    total = beta_k.shape[2]
    rows = beta_k.shape[1]
    per_atom = dmat.shape[1]
    layout = Layout(groups, displaced.shape[0], per_atom, total)

    beta_k, beta_kq = jnp.transpose(beta_k, (0, 2, 1)), jnp.transpose(beta_kq, (0, 2, 1))
    if groups == RING * CORE_Y:
        return fused(layout, psi_k, send_index, recv_index, beta_k, beta_kq, displaced, mode, g_k, g_kq, dmat)

    packed = pack_rows(send_index.reshape(1, -1), psi_k)
    arrived = lax.all_to_all(packed, "ga", split_axis=0, concat_axis=0, tiled=True)

    rank = jnp.sum((displaced[None, :] < displaced[:, None]).astype(jnp.int32), axis=1)
    place = rank[None, :] == jnp.arange(displaced.shape[0], dtype=jnp.int32)[:, None]
    atoms = jnp.sum(jnp.where(place, displaced[None, :], 0), axis=1)
    moves = jnp.sum(jnp.where(place[None], mode[:, None, :], 0.0), axis=2)
    steps = jnp.tile(jnp.arange(per_atom, dtype=F32), displaced.shape[0])
    source = jnp.repeat(atoms.astype(F32) * per_atom, per_atom) + steps
    source = pad_rows(layout, source[None], -1.0)
    weights = pad_rows(layout, jnp.repeat(moves, per_atom, axis=1), 0.0)
    filler = jnp.zeros((8 - 1 - weights.shape[0], source.shape[1]), F32)
    info = jnp.concatenate([source, weights, filler], axis=0)
    coupling = block_coupling(layout, dmat, atoms)
    return separate_steps(
        layout, arrived, recv_index.reshape(1, -1), beta_k, beta_kq, info, g_k, g_kq, coupling
    )


def solution(mesh):
    in_specs = (
        P(None, "ga", None),
        P(None, "ga", None),
        P(None, "ga", None),
        P(None, "ga"),
        P(None, "ga"),
        P("ga", None, None),
        P("ga"),
        P(),
        P("pert"),
        P(None, "pert"),
    )
    out_specs = P("pert", "ga", None)
    return jax.shard_map(
        on_device, mesh=mesh, in_specs=in_specs, out_specs=out_specs, check_vma=False
    )
```
